128 devices in a mesh: seq: 8 (over z_hi, x), batch: 16 (over z_lo, y, core).
Axes of the slice: x: 4, y: 4, z: 4 (z_hi: 2, z_lo: 2; z = z_hi * 2 + z_lo), core: 2. Of those that a mesh axis runs over, the one named last changes fastest.
Arguments:
- attn_out: bfloat16 [65536, 2560], P(('seq', 'batch')), may hold values from -200 to 200
- out_grad: bfloat16 [65536, 2560], P(('seq', 'batch')), may hold values from -6 to 6
- master: float32 [2560, 2560], P(('seq', 'batch')), may hold values from -0.125 to 0.125
- moment_one: float32 [2560, 2560], P(('seq', 'batch')), may hold values from -4 to 4
- moment_two: float32 [2560, 2560], P(('seq', 'batch')), may hold values from 0.002 to 0.05
Outputs:
- input_grad: bfloat16 [65536, 2560], P(('seq', 'batch'))
- new_master: float32 [2560, 2560], P(('seq', 'batch'))
- new_moment_one: float32 [2560, 2560], P(('seq', 'batch'))
- new_moment_two: float32 [2560, 2560], P(('seq', 'batch'))
The draws below stay inside these ranges and needn't reach their ends.
All inputs are finite; a program needn't handle non-finite values.
Results may differ from the reference program's by a relative error of at most 0.01.
Values may be sent and summed in bfloat16 or wider, within the bound.
A program may use at most 128 MiB of HBM per device.

```python
import math
import jax
import jax.numpy as jnp
from jax import lax

DIN = 2560
DOUT = 2560
TOK_DEV = 512
STEP = 10
TOKENS = 65536


def draw_attn_out(key, part):
    blocks = TOKENS // TOK_DEV
    feature_width = DIN // blocks
    first_key, second_key = jax.random.split(jax.random.fold_in(key, 11), 2)
    ramp = jnp.arange(DIN, dtype=jnp.float32) / jnp.float32(DIN)
    values = jax.random.normal(first_key, (TOKENS, DIN), jnp.float32)
    column = 10.0 ** ramp
    pairing = jax.random.permutation(second_key, blocks)
    token_block = jnp.arange(TOKENS) // TOK_DEV
    feature_block = jnp.arange(DIN) // feature_width
    spike = jnp.where(pairing[token_block][:, None] == feature_block[None, :], 6.0, 1.0)
    result = jnp.clip(values * column[None, :] * spike, -200.0, 200.0)
    return result.astype(jnp.bfloat16)


def steps_of(rng, shape, pieces, least, largest):
    factor_of, own = 1.0, jax.random.fold_in(rng, 6)
    for dim, parts in pieces:
        heights = jnp.exp(jax.random.uniform(jax.random.fold_in(own, dim), (parts,), jnp.float32, least / len(pieces), largest / len(pieces)))
        factor_of = factor_of * jnp.repeat(heights, shape[dim] // parts).reshape([-1 if axis == dim else 1 for axis in range(len(shape))])
    return factor_of


def noise(stream_key, extent, spread, most, shards=(), kind=jnp.bfloat16):
    drawn = jax.random.normal(stream_key, extent, jnp.float32) * spread
    if len(shards) > 0:
        drawn = steps_of(stream_key, extent, shards, -0.22, 0.18) * drawn
    return jnp.clip(drawn, min=-most, max=most).astype(kind)


def setup_inputs(seed: int = 0) -> dict:
    key_list = jax.random.split(jax.random.key(seed), 6)
    attn_out = draw_attn_out(jax.random.fold_in(key_list[5], 71), 0)
    out_grad = noise(key_list[1], (TOKENS, DOUT), 1.0, 6.0, ((0, 128),))
    master = noise(key_list[2], (DIN, DOUT), DIN ** -0.5, 0.125, ((0, 128),), jnp.float32)
    moment_one = noise(key_list[3], (DIN, DOUT), 0.3, 4.0, ((0, 128),), jnp.float32)
    moment_two = jnp.clip(jnp.exp(math.log(0.05) - 3.218876 * jax.random.uniform(key_list[4], (DIN, DOUT), jnp.float32) ** steps_of(key_list[4], (DIN, DOUT), ((0, 128),), -0.2, 0.2)), 0.002, 0.05)
    return dict(attn_out=attn_out, out_grad=out_grad, master=master, moment_one=moment_one, moment_two=moment_two)


def reference(attn_out, out_grad, master, moment_one, moment_two):
    weight = master.astype(jnp.bfloat16)
    input_grad = lax.dot_general(out_grad, weight, (((1,), (1,)), ((), ())), preferred_element_type=jnp.float32).astype(jnp.bfloat16)
    weight_grad = lax.dot_general(attn_out, out_grad, (((0,), (0,)), ((), ())), preferred_element_type=jnp.float32)
    grad_norm = jnp.sqrt(jnp.sum(weight_grad * weight_grad)) + 1e-06
    limit = jnp.sqrt(jnp.float32(DIN * DOUT))
    clipped = weight_grad * jnp.minimum(jnp.float32(1.0), limit / grad_norm)
    new_one = 0.9 * moment_one + 0.1 * clipped
    new_two = 0.999 * moment_two + 0.001 * clipped * clipped
    first_hat = new_one / (1.0 - 0.9 ** STEP)
    second_hat = new_two / (1.0 - 0.999 ** STEP)
    new_master = master - 0.01 * (first_hat / (jnp.sqrt(second_hat) + 1e-08) + 0.1 * master)
    return (input_grad, new_master, new_one, new_two)
```

```python
import jax
import jax.numpy as jnp
from jax import lax
from jax.experimental import pallas as pl
from jax.experimental.pallas import tpu as pltpu
from jax.sharding import PartitionSpec as P

DIN = 2560
DOUT = 2560
STEP = 10
TOK = 512
HALF = DIN // 2
ROWS = 80
CHUNKS = 5
OWN = 20
WIDE = 640
BF = jnp.bfloat16
F32 = jnp.float32
MESH = pl.DeviceIdType.MESH
COPIES = 240
AXES = ("y", "x", "z")
SPLITS = ("x", "z", "y")

GATHER = (("x", "y", "z"), ("y", "z", "x"), ("z", "y", "x"), ("x", "z", "y"), ("y", "z", "x"))
SCATTER = (("z", "y", "x"), ("x", "y", "z"), ("y", "z", "x"), ("z", "y", "x"), ("x", "z", "y"))

ORDER = (
    ("p1", 2), ("p1", 1), ("p1", 4), ("p1", 0), ("tr2",), ("rh", 0), ("pre",), ("ags", 3), ("ags", 1),
    ("rh", 2), ("ags", 2), ("rh", 1), ("p1", 3), ("rhm", 0), ("agm", 2), ("rhm", 1), ("rhm", 2), ("agm", 1),
    ("ags", 0), ("agm", 3), ("rm", 0), ("ags", 4), ("agmf", 1), ("rh", 3), ("rh", 4), ("agmf", 2), ("rmm", 0),
    ("rm", 1), ("agm", 0), ("agmf", 3), ("agh", 1), ("rhm", 3), ("rhm", 4), ("rm", 2), ("rmm", 1), ("rs", 0),
    ("agh", 3), ("rm", 4), ("agm", 4), ("agmf", 0), ("rm", 3), ("rmm", 2), ("aghf", 1), ("rmm", 4), ("aghf", 3),
    ("agmf", 4), ("rs", 1), ("agh", 2), ("rmm", 3), ("rs", 4), ("agh", 4), ("rs", 2), ("rs", 3), ("rz", 0),
    ("rz", 1), ("agh", 0), ("dx", 1), ("aghf", 2), ("rz", 2), ("rz", 3), ("rz", 4), ("fin",), ("n", 1),
    ("aghf", 4), ("aghf", 0), ("dx", 3), ("n", 2), ("dx", 2), ("dx", 4), ("n", 3), ("dx", 0), ("end",),
)


def where(chunk, chosen):
    every = pl.ds(0, 2)
    y_col, y_row = chosen.get("y", (every, every))
    z_col, z_row = chosen.get("z", (every, every))
    return (chunk, y_col, z_col, chosen.get("x", pl.ds(0, 4)), z_row, y_row)


DIMS = (("y", 0, 2), ("z", 0, 2), ("x", 0, 4), ("z", 1, 2), ("y", 1, 2))


def landing_shape(gone):
    return (3, *(size for axis, _, size in DIMS if axis not in gone), ROWS, 128)


def halves(axis):
    if axis == "x":
        return pl.ds(0, 2), pl.ds(2, 2)
    return (pl.ds(0, 2), pl.ds(0, 1)), (pl.ds(0, 2), pl.ds(1, 1))


class Body:
    def __init__(self, refs):
        (
            self.attn, self.og, self.master,
            self.dx, self.shard, self.norm,
            self.attn_v, self.attn_t, self.og_v, self.acc, self.grad, self.full, self.r_small, self.dx_acc,
            self.mst, self.give_w, self.stage, self.block, self.summed, self.pieces,
            self.norm_src, self.norm_in,
            self.load_sem, self.send, self.recv, self.pre_recv, self.fin_recv,
            *landings,
        ) = refs
        self.r_large, self.r_mid = landings[:CHUNKS], landings[CHUNKS:]
        self.used = 0
        self.sent = []
        self.late = []
        self.live = {}
        seq = lax.axis_index("seq")
        batch = lax.axis_index("batch")
        self.zh = seq // 4
        self.core = batch % 2
        self.zl = batch // 8
        self.at = {"x": seq % 4, "y": (batch // 2) % 4, "z": self.zh * 2 + self.zl}

    def device(self, x, y, z, core):
        return ((z // 2) * 4 + x, ((z % 2) * 4 + y) * 2 + core)

    def shifted(self, axis, by):
        return (self.at[axis] + by) % 4

    def peer(self, axis, by):
        place = dict(self.at)
        place[axis] = self.shifted(axis, by)
        return self.device(place["x"], place["y"], place["z"], self.core)

    def partner(self):
        return self.device(self.at["x"], self.at["y"], self.at["z"], 1 - self.core)

    def place(self, axis, by=0):
        at = self.shifted(axis, by)
        if axis == "x":
            return at
        if axis == "y":
            return (at % 2, at // 2)
        turned = (at + 2 * self.core) % 4
        col = turned // 2
        return (col, turned + col * (3 - 2 * turned))

    def copy(self, src, dst, device):
        n = self.used
        self.used += 1
        c = pltpu.make_async_remote_copy(
            src_ref=src, dst_ref=dst, send_sem=self.send.at[n], recv_sem=self.recv.at[n],
            device_id=device, device_id_type=MESH,
        )
        c.start()
        self.sent.append(c)
        return c

    def worker_place(self, q):
        z_col = q % 2
        turned = self.zl if z_col == 0 else 3 - self.zl
        return 2 * (self.at["y"] // 2) + q // 2, (turned + 2 * self.zh) % 4, self.zh

    def owner_place(self, i):
        z_row = self.place("z")[1]
        return 2 * (self.at["y"] // 2) + i // 2, 2 * self.core + z_row, i % 2

    def exchange(self, src, dst, recv, place):
        y, z, core = place
        n = self.used
        self.used += 1
        away = pltpu.make_async_remote_copy(
            src_ref=src, dst_ref=dst, send_sem=self.send.at[n], recv_sem=recv,
            device_id=self.device(self.at["x"], y, z, core), device_id_type=MESH,
        )
        here = pltpu.make_async_copy(src, dst, recv)
        mine = (y == self.at["y"]) & (z == self.at["z"]) & (core == self.core)
        pl.when(mine)(here.start)
        pl.when(jnp.logical_not(mine))(away.start)
        self.late.append((jnp.logical_not(mine), away))

    def exchanged(self, like, dst, recv):
        pltpu.make_async_remote_copy(
            src_ref=like, dst_ref=dst, send_sem=self.send.at[0], recv_sem=recv,
            device_id=self.partner(), device_id_type=MESH,
        ).wait_recv()

    def run(self):
        half = pl.multiple_of(self.core * HALF, 128)
        other = pl.multiple_of((1 - self.core) * HALF, 128)
        loads = [
            pltpu.make_async_copy(self.master, self.mst, self.load_sem.at[0]),
            pltpu.make_async_copy(self.attn.at[:, pl.ds(half, HALF)], self.attn_v.at[0], self.load_sem.at[1]),
            pltpu.make_async_copy(self.og, self.og_v.at[pl.ds(0, TOK)], self.load_sem.at[2]),
        ]
        for load in loads:
            load.start()
        barrier = pltpu.get_barrier_semaphore()
        greeted = [self.partner()]
        for axis in AXES:
            greeted += [self.peer(axis, by) for by in (1, 2, 3)]
        for q in range(4):
            for place in (self.worker_place(q), self.owner_place(q)):
                greeted.append(self.device(self.at["x"], *place))
        for device in greeted:
            pl.semaphore_signal(barrier, inc=1, device_id=device, device_id_type=MESH)
        loads[0].wait()
        for q in range(4):
            self.give_w[q] = jnp.concatenate(
                [self.mst[:, 512 * j + 128 * q : 512 * j + 128 * (q + 1)] for j in range(CHUNKS)], axis=1
            ).astype(BF)
        loads[1].wait()
        self.transpose(0)
        pl.semaphore_wait(barrier, len(greeted))

        self.swap_attn = self.copy(
            self.attn.at[:, pl.ds(other, HALF)], self.attn_v.at[1], self.partner()
        )
        slot = (self.at["y"] % 2) * 2 + self.core
        for q in range(4):
            self.exchange(
                self.give_w.at[q], self.stage.at[slot], self.pre_recv.at[slot], self.worker_place(q)
            )
        self.swap_og = [
            self.copy(
                self.og.at[:, pl.ds(512 * j, 512)], self.og_v.at[pl.ds(TOK, TOK), pl.ds(512 * j, 512)],
                self.partner(),
            )
            for j in range(CHUNKS)
        ]
        loads[2].wait()

        sums = [step for step in ORDER if step[0] == "dx"]
        for step in ORDER:
            name = step[0]
            if step == sums[0]:
                name = "dx_first"
            elif step == sums[-1]:
                name = "dx_last"
            elif step in sums:
                name = "dx_more"
            getattr(self, name)(*step[1:])

        for c in self.sent:
            c.wait_send()
        for go, c in self.late:
            pl.when(go)(c.wait_send)

    def transpose(self, which):
        def body(i, carry):
            lanes = pl.ds(pl.multiple_of(i * 128, 128), 128)
            self.attn_t[which, lanes, :] = self.attn_v[which, :, lanes].T
            return carry

        lax.fori_loop(0, HALF // 128, body, 0)

    def tr2(self):
        self.swap_attn.wait_recv()
        self.transpose(1)

    def p1(self, j):
        self.acc[j] = jnp.dot(
            self.attn_t[0], self.og_v[pl.ds(0, TOK), pl.ds(512 * j, 512)], preferred_element_type=F32
        )

    def pre(self):
        for s in range(4):
            self.exchanged(self.give_w.at[0], self.stage.at[s], self.pre_recv.at[s])
            self.block[OWN * s : OWN * (s + 1), :] = self.stage[s].astype(F32)
        here = {axis: self.place(axis) for axis in AXES}
        for j in range(CHUNKS):
            self.full[where(j, here)] = self.block[:, 128 * j : 128 * (j + 1)].astype(BF)

    def ags(self, j):
        axis = GATHER[j][2]
        here = self.full.at[where(j, {a: self.place(a) for a in AXES})]
        self.live["ags", j] = [self.copy(here, here, self.peer(axis, by)) for by in (1, 3, 2)]

    def ring(self, j, axis, fixed, key):
        chosen = {a: self.place(a) for a in fixed}
        split = next(a for a in SPLITS if a != axis and a not in chosen)
        first, second = halves(split)

        def part(by, rows):
            return self.full.at[where(j, {**chosen, axis: self.place(axis, by), split: rows})]

        ahead, behind = self.peer(axis, 1), self.peer(axis, 3)
        top_ahead = self.copy(part(0, first), part(0, first), ahead)
        low_behind = self.copy(part(0, second), part(0, second), behind)
        low_ahead = self.copy(part(0, second), part(0, second), ahead)
        top_behind = self.copy(part(0, first), part(0, first), behind)
        self.live[key] = (top_ahead, low_behind, low_ahead, top_behind, part, first, second)

    def forward(self, axis, key):
        top_ahead, low_behind, low_ahead, top_behind, part, first, second = self.live[key]
        top_ahead.wait_recv()
        on = self.copy(part(3, first), part(3, first), self.peer(axis, 1))
        low_behind.wait_recv()
        back = self.copy(part(1, second), part(1, second), self.peer(axis, 3))
        self.live[key] = (low_ahead, top_behind, on, back)

    def finish(self, key):
        for c in self.live[key]:
            c.wait_recv()

    def agm(self, j):
        self.finish(("ags", j))
        self.ring(j, GATHER[j][1], (GATHER[j][0],), ("agm", j))

    def agmf(self, j):
        self.forward(GATHER[j][1], ("agm", j))

    def agh(self, j):
        self.finish(("agm", j))
        self.ring(j, GATHER[j][0], (), ("agh", j))

    def aghf(self, j):
        self.forward(GATHER[j][0], ("agh", j))

    def dx_dot(self, j, rows):
        left = self.og_v[rows, pl.ds(512 * j, 512)]
        right = jnp.concatenate(
            [self.full[j, q // 2, q % 2].reshape(HALF, 128) for q in range(4)], axis=1
        )
        return lax.dot_general(left, right, (((1,), (1,)), ((), ())), preferred_element_type=F32)

    def dx_first(self, j):
        self.finish(("agh", j))
        self.dx_acc[...] = self.dx_dot(j, pl.ds(0, 2 * TOK))

    def dx_more(self, j):
        self.finish(("agh", j))
        self.dx_acc[...] += self.dx_dot(j, pl.ds(0, 2 * TOK))

    def dx_last(self, j):
        self.finish(("agh", j))
        half = pl.ds(pl.multiple_of(self.core * HALF, 128), HALF)
        theirs, ours = pl.ds(TOK, TOK), pl.ds(0, TOK)
        self.attn_v[1] = (self.dx_acc[theirs, :] + self.dx_dot(j, theirs)).astype(BF)
        give = self.copy(self.attn_v.at[1], self.dx.at[:, half], self.partner())
        self.attn_v[0] = (self.dx_acc[ours, :] + self.dx_dot(j, ours)).astype(BF)
        keep = pltpu.make_async_copy(self.attn_v.at[0], self.dx.at[:, half], self.load_sem.at[3])
        keep.start()
        give.wait_recv()
        keep.wait()

    def rh(self, j):
        self.swap_og[j].wait_recv()
        v = self.acc[j] + jnp.dot(
            self.attn_t[1], self.og_v[pl.ds(TOK, TOK), pl.ds(512 * j, 512)], preferred_element_type=F32
        )
        v = v.astype(BF)
        for q in range(4):
            self.grad[j, q // 2, q % 2] = v[:, 128 * q : 128 * (q + 1)].reshape(4, 2, 2, ROWS, 128)
        self.reduce(j, SCATTER[j][0], (), self.r_large[j], ("rh", j))

    def reduce(self, j, axis, fixed, landing, key):
        chosen = {a: self.place(a) for a in fixed}
        split = next(a for a in SPLITS if a != axis and a not in chosen)
        first, second = halves(split)
        ahead, behind = self.peer(axis, 1), self.peer(axis, 3)

        def part(by, rows):
            return where(j, {**chosen, axis: self.place(axis, by), split: rows})

        def land(slot, rows):
            index = [slot]
            for a, k, size in DIMS:
                if a == split:
                    index.append(rows if a == "x" else rows[k])
                elif a != axis and a not in chosen:
                    index.append(pl.ds(0, size))
            return tuple(index)

        far_ahead = self.copy(self.grad.at[part(2, first)], landing.at[land(0, first)], ahead)
        far_behind = self.copy(self.grad.at[part(2, second)], landing.at[land(0, second)], behind)
        near_ahead = self.copy(self.grad.at[part(1, second)], landing.at[land(1, second)], ahead)
        near_behind = self.copy(self.grad.at[part(3, first)], landing.at[land(2, first)], behind)
        self.live[key] = (far_ahead, far_behind, near_ahead, near_behind, part, land, first, second)

    def pass_on(self, axis, landing, key):
        far_ahead, far_behind, near_ahead, near_behind, part, land, first, second = self.live[key]
        far_ahead.wait_recv()
        at = part(1, first)
        self.grad[at] = (self.grad[at].astype(F32) + landing[land(0, first)].astype(F32)).astype(BF)
        on = self.copy(self.grad.at[at], landing.at[land(1, first)], self.peer(axis, 1))
        far_behind.wait_recv()
        at = part(3, second)
        self.grad[at] = (self.grad[at].astype(F32) + landing[land(0, second)].astype(F32)).astype(BF)
        back = self.copy(self.grad.at[at], landing.at[land(2, second)], self.peer(axis, 3))
        self.live[key] = (near_ahead, near_behind, on, back)

    def rhm(self, j):
        self.pass_on(SCATTER[j][0], self.r_large[j], ("rh", j))

    def rm(self, j):
        self.finish(("rh", j))
        large, mid, small = SCATTER[j]
        at = where(j, {large: self.place(large)})
        landed = self.r_large[j]
        total = self.grad[at].astype(F32) + landed[1].astype(F32)
        self.grad[at] = (total + landed[2].astype(F32)).astype(BF)
        self.reduce(j, mid, (large,), self.r_mid[j], ("rm", j))

    def rmm(self, j):
        self.pass_on(SCATTER[j][1], self.r_mid[j], ("rm", j))

    def rs(self, j):
        self.finish(("rm", j))
        large, mid, small = SCATTER[j]
        chosen = {large: self.place(large), mid: self.place(mid)}
        at = where(j, chosen)
        landed = self.r_mid[j]
        total = self.grad[at].astype(F32) + landed[1].astype(F32)
        self.grad[at] = (total + landed[2].astype(F32)).astype(BF)
        self.live["rs", j] = [
            self.copy(
                self.grad.at[where(j, {**chosen, small: self.place(small, by)})],
                self.r_small.at[j, by - 1],
                self.peer(small, by),
            )
            for by in (1, 3, 2)
        ]

    def rz(self, j):
        self.finish(("rs", j))
        total = self.grad[where(j, {a: self.place(a) for a in AXES})].astype(F32)
        for s in range(3):
            total += self.r_small[j, s].astype(F32)
        self.summed[:, 128 * j : 128 * (j + 1)] = total

    def fin(self):
        total = self.summed[...]
        squares = jnp.sum(total * total, axis=(0, 1), keepdims=True)
        self.norm_src[0] = jnp.broadcast_to(squares, (8, 128))
        self.norm_last = [self.copy(self.norm_src.at[0], self.norm_in.at[0], self.partner())]
        piece = self.place("y")[0] * 2 + self.place("z")[0]
        for i in range(4):
            self.pieces[i] = self.summed[OWN * i : OWN * (i + 1), :]
            self.exchange(
                self.pieces.at[i], self.shard.at[piece], self.fin_recv.at[piece], self.owner_place(i)
            )

    def norm_total(self, k):
        total = self.norm_src[k - 1]
        first = 0 if k == 1 else 3 * k - 5
        for c in self.norm_last:
            c.wait_recv()
        for s in range(len(self.norm_last)):
            total += self.norm_in[first + s]
        return total

    def n(self, k):
        self.norm_src[k] = self.norm_total(k)
        axis = AXES[k - 1]
        self.norm_last = [
            self.copy(self.norm_src.at[k], self.norm_in.at[3 * k - 3 + by], self.peer(axis, by))
            for by in (1, 2, 3)
        ]

    def end(self):
        self.norm_src[4] = self.norm_total(4)
        out = pltpu.make_async_copy(self.norm_src.at[4], self.norm, self.load_sem.at[4])
        out.start()
        for q in range(4):
            self.exchanged(self.pieces.at[0], self.shard.at[q], self.fin_recv.at[q])
        out.wait()


def kernel(*refs):
    Body(refs).run()


def update(*refs):
    dx, *shard_in, dx_out, new_master, new_one, new_two = refs[:10]
    held, *held_in, put_master, put_one, put_two, into_sem, out_sem, small_in, small_out = refs[10:]
    parts = 4
    rows = [pl.ds(TOK // parts * i, TOK // parts) for i in range(parts)]
    into = [pltpu.make_async_copy(dx.at[rows[i]], held.at[i], into_sem.at[i]) for i in range(parts)]
    out = [pltpu.make_async_copy(held.at[i], dx_out.at[rows[i]], out_sem.at[i]) for i in range(parts)]
    loads = [pltpu.make_async_copy(a, b, small_in.at[i]) for i, (a, b) in enumerate(zip(shard_in, held_in))]
    for c in loads[:2] + into[:2] + loads[2:] + into[2:]:
        c.start()
    shard, norm, master, one, two = held_in
    for c in loads[:2] + into[:2]:
        c.wait()
    out[0].start()
    out[1].start()
    limit = jnp.sqrt(jnp.float32(DIN * DOUT))
    clip = jnp.minimum(1.0, limit / (jnp.sqrt(norm[0:1, 0:1]) + 1e-06))
    for c in loads[2:] + into[2:]:
        c.wait()
    out[2].start()
    out[3].start()
    for q in range(4):
        for j in range(CHUNKS):
            cols = slice(512 * j + 128 * q, 512 * j + 128 * (q + 1))
            clipped = shard[q, :, 128 * j : 128 * (j + 1)] * clip
            weight = master[:, cols]
            first = 0.9 * one[:, cols] + 0.1 * clipped
            second = 0.999 * two[:, cols] + 0.001 * clipped * clipped
            first_hat = first / (1.0 - 0.9**STEP)
            second_hat = second / (1.0 - 0.999**STEP)
            put_one[:, cols] = first
            put_two[:, cols] = second
            put_master[:, cols] = weight - 0.01 * (
                first_hat / (jnp.sqrt(second_hat) + 1e-08) + 0.1 * weight
            )
    for i, (a, b) in enumerate(((put_one, new_one), (put_two, new_two), (put_master, new_master))):
        c = pltpu.make_async_copy(a, b, small_out.at[i])
        c.start()
        out.append(c)
    for c in out:
        c.wait()


def on_device(attn_out, out_grad, master, moment_one, moment_two):
    anywhere = pl.BlockSpec(memory_space=pl.ANY)
    vmem = pl.BlockSpec(memory_space=pltpu.VMEM)
    dx, shard, norm = pl.pallas_call(
        kernel,
        out_shape=(
            jax.ShapeDtypeStruct((TOK, DIN), BF),
            jax.ShapeDtypeStruct((4, OWN, WIDE), F32),
            jax.ShapeDtypeStruct((8, 128), F32),
        ),
        in_specs=[anywhere] * 3,
        out_specs=(anywhere,) * 3,
        scratch_shapes=[
            pltpu.VMEM((2, TOK, HALF), BF),
            pltpu.VMEM((2, HALF, TOK), BF),
            pltpu.VMEM((2 * TOK, DOUT), BF),
            pltpu.VMEM((CHUNKS, HALF, 512), F32),
            pltpu.VMEM((CHUNKS, 2, 2, 4, 2, 2, ROWS, 128), BF),
            pltpu.VMEM((CHUNKS, 2, 2, 4, 2, 2, ROWS, 128), BF),
            pltpu.VMEM((CHUNKS, 3, ROWS, 128), BF),
            pltpu.VMEM((2 * TOK, HALF), F32),
            pltpu.VMEM((OWN, DOUT), F32),
            pltpu.VMEM((4, OWN, WIDE), BF),
            pltpu.VMEM((4, OWN, WIDE), BF),
            pltpu.VMEM((ROWS, WIDE), F32),
            pltpu.VMEM((ROWS, WIDE), F32),
            pltpu.VMEM((4, OWN, WIDE), F32),
            pltpu.VMEM((5, 8, 128), F32),
            pltpu.VMEM((10, 8, 128), F32),
            pltpu.SemaphoreType.DMA((5,)),
            pltpu.SemaphoreType.DMA((COPIES,)),
            pltpu.SemaphoreType.DMA((COPIES,)),
            pltpu.SemaphoreType.DMA((4,)),
            pltpu.SemaphoreType.DMA((4,)),
            *(pltpu.VMEM(landing_shape(axes[:1]), BF) for axes in SCATTER),
            *(pltpu.VMEM(landing_shape(axes[:2]), BF) for axes in SCATTER),
        ],
        compiler_params=pltpu.CompilerParams(
            collective_id=0, has_side_effects=True, vmem_limit_bytes=66_000_000
        ),
        cost_estimate=pl.CostEstimate(
            flops=4 * TOK * DIN * DOUT, bytes_accessed=40_000_000, transcendentals=0
        ),
        name="step",
    )(attn_out, out_grad, master)
    part = jax.ShapeDtypeStruct((OWN, DOUT), F32)
    row = pltpu.VMEM((OWN, DOUT), F32)
    return pl.pallas_call(
        update,
        out_shape=(jax.ShapeDtypeStruct((TOK, DIN), BF), part, part, part),
        in_specs=[anywhere] * 6,
        out_specs=(anywhere,) * 4,
        scratch_shapes=[
            pltpu.VMEM((4, TOK // 4, DIN), BF),
            pltpu.VMEM((4, OWN, WIDE), F32),
            pltpu.VMEM((8, 128), F32),
            *(row,) * 6,
            pltpu.SemaphoreType.DMA((4,)),
            pltpu.SemaphoreType.DMA((4,)),
            pltpu.SemaphoreType.DMA((5,)),
            pltpu.SemaphoreType.DMA((3,)),
        ],
        name="update",
    )(dx, shard, norm, master, moment_one, moment_two)


def solution(mesh):
    split = P(("seq", "batch"), None)
    return jax.shard_map(
        on_device, mesh=mesh, in_specs=(split,) * 5, out_specs=(split,) * 4, check_vma=False
    )
```

```python
import jax
import jax.numpy as jnp
from jax import lax
from jax.experimental import pallas as pl
from jax.experimental.pallas import tpu as pltpu
from jax.sharding import PartitionSpec as P

DIN = 2560
DOUT = 2560
STEP = 10
TOK = 512
HALF = DIN // 2
ROWS = 80
CHUNKS = 5
OWN = 20
WIDE = 640
BF = jnp.bfloat16
F32 = jnp.float32
MESH = pl.DeviceIdType.MESH
RECEIVES = 84
SENDS = 19
AXES = ("y", "x", "z")
SPLITS = ("x", "z", "y")

GATHER = (("x", "y", "z"), ("y", "z", "x"), ("z", "y", "x"), ("x", "z", "y"), ("y", "z", "x"))
SCATTER = (("z", "y", "x"), ("x", "y", "z"), ("y", "z", "x"), ("z", "y", "x"), ("x", "z", "y"))

ORDER = (
    ("p1", 2), ("p1", 1), ("p1", 4), ("p1", 0), ("tr2",), ("rh", 0), ("pre",), ("ags", 3), ("ags", 1),
    ("rh", 2), ("ags", 2), ("rh", 1), ("p1", 3), ("rhm", 0), ("agm", 2), ("rhm", 1), ("rhm", 2), ("agm", 1),
    ("ags", 0), ("agm", 3), ("rm", 0), ("ags", 4), ("agmf", 1), ("rh", 3), ("rh", 4), ("agmf", 2), ("rmm", 0),
    ("rm", 1), ("agm", 0), ("agmf", 3), ("agh", 1), ("rhm", 3), ("rhm", 4), ("rm", 2), ("rmm", 1), ("rs", 0),
    ("agh", 3), ("rm", 4), ("agm", 4), ("agmf", 0), ("rm", 3), ("rmm", 2), ("aghf", 1), ("rmm", 4), ("aghf", 3),
    ("agmf", 4), ("rs", 1), ("agh", 2), ("rmm", 3), ("rs", 4), ("agh", 4), ("rs", 2), ("rs", 3), ("rz", 0),
    ("rz", 1), ("agh", 0), ("dx", 1), ("aghf", 2), ("rz", 2), ("rz", 3), ("rz", 4), ("fin",), ("n", 1),
    ("aghf", 4), ("aghf", 0), ("dx", 3), ("n", 2), ("dx", 2), ("dx", 4), ("n", 3), ("dx", 0), ("end",),
)


def where(chunk, chosen):
    every = pl.ds(0, 2)
    y_col, y_row = chosen.get("y", (every, every))
    z_col, z_row = chosen.get("z", (every, every))
    return (chunk, y_col, z_col, chosen.get("x", pl.ds(0, 4)), z_row, y_row)


DIMS = (("y", 0, 2), ("z", 0, 2), ("x", 0, 4), ("z", 1, 2), ("y", 1, 2))


def landing_shape(gone):
    return (3, *(size for axis, _, size in DIMS if axis not in gone), ROWS, 128)


def halves(axis):
    if axis == "x":
        return pl.ds(0, 2), pl.ds(2, 2)
    return (pl.ds(0, 2), pl.ds(0, 1)), (pl.ds(0, 2), pl.ds(1, 1))


class Body:
    def __init__(self, refs):
        (
            self.attn, self.og, self.master,
            self.dx, self.shard, self.norm,
            self.attn_v, self.attn_t, self.og_v, self.acc, self.grad, self.full, self.r_small, self.dx_acc,
            self.mst, self.give_w, self.stage, self.block, self.summed, self.pieces,
            self.norm_src, self.norm_in,
            self.load_sem, self.send, self.single, self.recv, self.pre_recv, self.fin_recv,
            *landings,
        ) = refs
        self.r_large, self.r_mid = landings[:CHUNKS], landings[CHUNKS:]
        self.used = 0
        self.singles = 0
        self.sent = []
        self.late = []
        self.live = {}
        seq = lax.axis_index("seq")
        batch = lax.axis_index("batch")
        self.zh = seq // 4
        self.core = batch % 2
        self.zl = batch // 8
        self.at = {"x": seq % 4, "y": (batch // 2) % 4, "z": self.zh * 2 + self.zl}

    def device(self, x, y, z, core):
        return ((z // 2) * 4 + x, ((z % 2) * 4 + y) * 2 + core)

    def shifted(self, axis, by):
        return (self.at[axis] + by) % 4

    def peer(self, axis, by):
        place = dict(self.at)
        place[axis] = self.shifted(axis, by)
        return self.device(place["x"], place["y"], place["z"], self.core)

    def partner(self):
        return self.device(self.at["x"], self.at["y"], self.at["z"], 1 - self.core)

    def place(self, axis, by=0):
        at = self.shifted(axis, by)
        if axis == "x":
            return at
        if axis == "y":
            return (at % 2, at // 2)
        turned = (at + 2 * self.core) % 4
        col = turned // 2
        return (col, turned + col * (3 - 2 * turned))

    def fresh(self):
        self.used += 1
        return self.used - 1

    def own_send(self):
        self.singles += 1
        return self.single.at[self.singles - 1]

    def copy(self, src, dst, device, recv=None, group=None):
        n = self.fresh() if recv is None else recv
        c = pltpu.make_async_remote_copy(
            src_ref=src, dst_ref=dst,
            send_sem=self.own_send() if group is None else self.send.at[group],
            recv_sem=self.recv.at[n], device_id=device, device_id_type=MESH,
        )
        c.start()
        if group is None:
            self.sent.append(c)
        return c

    def take(self, like, n):
        self.exchanged(like, like, self.recv.at[n])

    def drain(self):
        for group in range(9):
            blocks = self.full.at[:, :, :, pl.ds(0, 3)]
            if group % 3 == 1:
                blocks = self.full.at[:, pl.ds(0, 1), pl.ds(0, 1), pl.ds(0, 3)]
            if group % 3 == 2:
                one = pl.ds(0, 1)
                blocks = self.full.at[:, one, one, pl.ds(0, 3), one, one]
            if group > 5:
                blocks = self.norm_in.at[pl.ds(1, 3)]
            pltpu.make_async_remote_copy(
                src_ref=blocks, dst_ref=blocks, send_sem=self.send.at[group], recv_sem=self.recv.at[0],
                device_id=self.partner(), device_id_type=MESH,
            ).wait_send()

    def worker_place(self, q):
        z_col = q % 2
        turned = self.zl if z_col == 0 else 3 - self.zl
        return 2 * (self.at["y"] // 2) + q // 2, (turned + 2 * self.zh) % 4, self.zh

    def owner_place(self, i):
        z_row = self.place("z")[1]
        return 2 * (self.at["y"] // 2) + i // 2, 2 * self.core + z_row, i % 2

    def exchange(self, src, dst, recv, place):
        y, z, core = place
        away = pltpu.make_async_remote_copy(
            src_ref=src, dst_ref=dst, send_sem=self.own_send(), recv_sem=recv,
            device_id=self.device(self.at["x"], y, z, core), device_id_type=MESH,
        )
        here = pltpu.make_async_copy(src, dst, recv)
        mine = (y == self.at["y"]) & (z == self.at["z"]) & (core == self.core)
        pl.when(mine)(here.start)
        pl.when(jnp.logical_not(mine))(away.start)
        self.late.append((jnp.logical_not(mine), away))

    def exchanged(self, like, dst, recv):
        pltpu.make_async_remote_copy(
            src_ref=like, dst_ref=dst, send_sem=self.single.at[0], recv_sem=recv,
            device_id=self.partner(), device_id_type=MESH,
        ).wait_recv()

    def run(self):
        half = pl.multiple_of(self.core * HALF, 128)
        other = pl.multiple_of((1 - self.core) * HALF, 128)
        loads = [
            pltpu.make_async_copy(self.master, self.mst, self.load_sem.at[0]),
            pltpu.make_async_copy(self.attn.at[:, pl.ds(half, HALF)], self.attn_v.at[0], self.load_sem.at[1]),
            pltpu.make_async_copy(self.og, self.og_v.at[pl.ds(0, TOK)], self.load_sem.at[2]),
        ]
        for load in loads:
            load.start()
        barrier = pltpu.get_barrier_semaphore()
        greeted = [self.partner()]
        for axis in AXES:
            greeted += [self.peer(axis, by) for by in (1, 2, 3)]
        for q in range(4):
            for place in (self.worker_place(q), self.owner_place(q)):
                greeted.append(self.device(self.at["x"], *place))
        for device in greeted:
            pl.semaphore_signal(barrier, inc=1, device_id=device, device_id_type=MESH)
        loads[0].wait()
        for q in range(4):
            self.give_w[q] = jnp.concatenate(
                [self.mst[:, 512 * j + 128 * q : 512 * j + 128 * (q + 1)] for j in range(CHUNKS)], axis=1
            ).astype(BF)
        loads[1].wait()
        self.transpose(0)
        pl.semaphore_wait(barrier, len(greeted))

        part = HALF // 2
        self.swap_attn = [
            self.copy(
                self.attn.at[:, pl.ds(pl.multiple_of(other + part * i, 128), part)],
                self.attn_v.at[1, :, pl.ds(part * i, part)],
                self.partner(),
            )
            for i in range(2)
        ]
        slot = (self.at["y"] % 2) * 2 + self.core
        for q in range(4):
            self.exchange(
                self.give_w.at[q], self.stage.at[slot], self.pre_recv.at[slot], self.worker_place(q)
            )
        self.swap_og = [
            self.copy(
                self.og.at[:, pl.ds(512 * j, 512)], self.og_v.at[pl.ds(TOK, TOK), pl.ds(512 * j, 512)],
                self.partner(),
            )
            for j in range(CHUNKS)
        ]
        loads[2].wait()

        sums = [step for step in ORDER if step[0] == "dx"]
        for step in ORDER:
            name = step[0]
            if step == sums[0]:
                name = "dx_first"
            elif step == sums[-1]:
                name = "dx_last"
            elif step in sums:
                name = "dx_more"
            getattr(self, name)(*step[1:])

        self.drain()
        for c in self.sent:
            c.wait_send()
        for go, c in self.late:
            pl.when(go)(c.wait_send)

    def transpose(self, which, first=0, last=10):
        def body(i, carry):
            lanes = pl.ds(pl.multiple_of(i * 128, 128), 128)
            self.attn_t[which, lanes, :] = self.attn_v[which, :, lanes].T
            return carry

        lax.fori_loop(first, last, body, 0)

    def tr2(self):
        for i in range(2):
            self.swap_attn[i].wait_recv()
            self.transpose(1, 5 * i, 5 * i + 5)

    def p1(self, j):
        self.acc[j] = jnp.dot(
            self.attn_t[0], self.og_v[pl.ds(0, TOK), pl.ds(512 * j, 512)], preferred_element_type=F32
        )

    def pre(self):
        for s in range(4):
            self.exchanged(self.give_w.at[0], self.stage.at[s], self.pre_recv.at[s])
            self.block[OWN * s : OWN * (s + 1), :] = self.stage[s].astype(F32)
        here = {axis: self.place(axis) for axis in AXES}
        for j in range(CHUNKS):
            self.full[where(j, here)] = self.block[:, 128 * j : 128 * (j + 1)].astype(BF)

    def ags(self, j):
        axis = GATHER[j][2]
        here = self.full.at[where(j, {a: self.place(a) for a in AXES})]
        n = self.fresh()
        for by in (1, 3, 2):
            self.copy(here, here, self.peer(axis, by), n, 2)
        self.live["ags", j] = (n, self.r_small.at[j])

    def ring(self, j, axis, fixed, key, group, both):
        chosen = {a: self.place(a) for a in fixed}
        split = next(a for a in SPLITS if a != axis and a not in chosen)
        first, second = halves(split)

        def part(by, rows):
            return self.full.at[where(j, {**chosen, axis: self.place(axis, by), split: rows})]

        ahead, behind = self.peer(axis, 1), self.peer(axis, 3)
        n = self.fresh()
        top_ahead = self.copy(part(0, first), part(0, first), ahead, None, group)
        low_behind = self.copy(part(0, second), part(0, second), behind, None, group)
        self.copy(part(0, second), part(0, second), ahead, n, group)
        self.copy(part(0, first), part(0, first), behind, n, group)
        self.live[key] = (top_ahead, low_behind, part, first, second, n, group, both)

    def forward(self, axis, key):
        top_ahead, low_behind, part, first, second, n, group, both = self.live[key]
        top_ahead.wait_recv()
        self.copy(part(3, first), part(3, first), self.peer(axis, 1), n, group)
        low_behind.wait_recv()
        self.copy(part(1, second), part(1, second), self.peer(axis, 3), n, group)
        self.live[key] = (n, both)

    def finish(self, key):
        n, like = self.live[key]
        self.take(like, n)

    def agm(self, j):
        self.finish(("ags", j))
        self.ring(j, GATHER[j][1], (GATHER[j][0],), ("agm", j), 1, self.r_mid[j].at[pl.ds(0, 2)])

    def agmf(self, j):
        self.forward(GATHER[j][1], ("agm", j))

    def agh(self, j):
        self.finish(("agm", j))
        self.ring(j, GATHER[j][0], (), ("agh", j), 0, self.r_large[j].at[pl.ds(0, 2)])

    def aghf(self, j):
        self.forward(GATHER[j][0], ("agh", j))

    def dx_dot(self, j, rows, first=0, last=HALF):
        left = self.og_v[rows, pl.ds(512 * j, 512)]
        right = jnp.concatenate(
            [self.full[j, q // 2, q % 2].reshape(HALF, 128)[first:last] for q in range(4)], axis=1
        )
        return lax.dot_general(left, right, (((1,), (1,)), ((), ())), preferred_element_type=F32)

    def dx_first(self, j):
        self.finish(("agh", j))
        self.dx_acc[...] = self.dx_dot(j, pl.ds(0, 2 * TOK))

    def dx_more(self, j):
        self.finish(("agh", j))
        self.dx_acc[...] += self.dx_dot(j, pl.ds(0, 2 * TOK))

    def dx_last(self, j):
        self.finish(("agh", j))
        start = self.core * HALF
        gives, keeps = [], []
        for which, rows in ((1, pl.ds(TOK, TOK)), (0, pl.ds(0, TOK))):
            for i, (first, last) in enumerate(((0, 512), (512, 1024), (1024, HALF))):
                cols = pl.ds(first, last - first)
                done = self.dx_acc[rows, cols] + self.dx_dot(j, rows, first, last)
                self.attn_v[which, :, cols] = done.astype(BF)
                src = self.attn_v.at[which, :, cols]
                to = self.dx.at[:, pl.ds(pl.multiple_of(start + first, 128), last - first)]
                if which:
                    gives.append(self.copy(src, to, self.partner()))
                else:
                    keep = pltpu.make_async_copy(src, to, self.load_sem.at[5 + i])
                    keep.start()
                    keeps.append(keep)
        for c in gives:
            c.wait_recv()
        for c in keeps:
            c.wait()

    def rh(self, j):
        self.swap_og[j].wait_recv()
        v = self.acc[j] + jnp.dot(
            self.attn_t[1], self.og_v[pl.ds(TOK, TOK), pl.ds(512 * j, 512)], preferred_element_type=F32
        )
        v = v.astype(BF)
        for q in range(4):
            self.grad[j, q // 2, q % 2] = v[:, 128 * q : 128 * (q + 1)].reshape(4, 2, 2, ROWS, 128)
        self.reduce(j, SCATTER[j][0], (), self.r_large[j], ("rh", j), 3)

    def reduce(self, j, axis, fixed, landing, key, group):
        chosen = {a: self.place(a) for a in fixed}
        split = next(a for a in SPLITS if a != axis and a not in chosen)
        first, second = halves(split)
        ahead, behind = self.peer(axis, 1), self.peer(axis, 3)

        def part(by, rows):
            return where(j, {**chosen, axis: self.place(axis, by), split: rows})

        def land(slot, rows):
            index = [slot]
            for a, k, size in DIMS:
                if a == split:
                    index.append(rows if a == "x" else rows[k])
                elif a != axis and a not in chosen:
                    index.append(pl.ds(0, size))
            return tuple(index)

        n = self.fresh()

        def send(by, rows, slot, device, recv):
            return self.copy(
                self.grad.at[part(by, rows)], landing.at[land(slot, rows)], device, recv, group
            )

        far_ahead = send(2, first, 0, ahead, None)
        far_behind = send(2, second, 0, behind, None)
        send(1, second, 1, ahead, n)
        send(3, first, 2, behind, n)
        self.live[key] = (far_ahead, far_behind, part, land, first, second, n, send)

    def pass_on(self, axis, landing, key):
        far_ahead, far_behind, part, land, first, second, n, send = self.live[key]
        far_ahead.wait_recv()
        at = part(1, first)
        self.grad[at] = (self.grad[at].astype(F32) + landing[land(0, first)].astype(F32)).astype(BF)
        send(1, first, 1, self.peer(axis, 1), n)
        far_behind.wait_recv()
        at = part(3, second)
        self.grad[at] = (self.grad[at].astype(F32) + landing[land(0, second)].astype(F32)).astype(BF)
        send(3, second, 2, self.peer(axis, 3), n)
        self.live[key] = (n, landing.at[pl.ds(0, 2)])

    def rhm(self, j):
        self.pass_on(SCATTER[j][0], self.r_large[j], ("rh", j))

    def rm(self, j):
        self.finish(("rh", j))
        large, mid, small = SCATTER[j]
        at = where(j, {large: self.place(large)})
        landed = self.r_large[j]
        total = self.grad[at].astype(F32) + landed[1].astype(F32)
        self.grad[at] = (total + landed[2].astype(F32)).astype(BF)
        self.reduce(j, mid, (large,), self.r_mid[j], ("rm", j), 4)

    def rmm(self, j):
        self.pass_on(SCATTER[j][1], self.r_mid[j], ("rm", j))

    def rs(self, j):
        self.finish(("rm", j))
        large, mid, small = SCATTER[j]
        chosen = {large: self.place(large), mid: self.place(mid)}
        at = where(j, chosen)
        landed = self.r_mid[j]
        total = self.grad[at].astype(F32) + landed[1].astype(F32)
        self.grad[at] = (total + landed[2].astype(F32)).astype(BF)
        n = self.fresh()
        for by in (1, 3, 2):
            at = where(j, {**chosen, small: self.place(small, by)})
            self.copy(self.grad.at[at], self.r_small.at[j, by - 1], self.peer(small, by), n, 5)
        self.live["rs", j] = (n, self.r_small.at[j])

    def rz(self, j):
        self.finish(("rs", j))
        total = self.grad[where(j, {a: self.place(a) for a in AXES})].astype(F32)
        for s in range(3):
            total += self.r_small[j, s].astype(F32)
        self.summed[:, 128 * j : 128 * (j + 1)] = total

    def fin(self):
        total = self.summed[...]
        squares = jnp.sum(total * total, axis=(0, 1), keepdims=True)
        self.norm_src[0] = jnp.broadcast_to(squares, (8, 128))
        self.norm_last = self.fresh()
        self.copy(self.norm_src.at[0], self.norm_in.at[0], self.partner(), self.norm_last)
        piece = self.place("y")[0] * 2 + self.place("z")[0]
        for i in range(4):
            self.pieces[i] = self.summed[OWN * i : OWN * (i + 1), :]
            self.exchange(
                self.pieces.at[i], self.shard.at[piece], self.fin_recv.at[piece], self.owner_place(i)
            )

    def norm_total(self, k):
        total = self.norm_src[k - 1]
        first, count = (0, 1) if k == 1 else (3 * k - 5, 3)
        self.take(self.norm_in.at[pl.ds(first, count)], self.norm_last)
        for s in range(count):
            total += self.norm_in[first + s]
        return total

    def n(self, k):
        self.norm_src[k] = self.norm_total(k)
        axis = AXES[k - 1]
        self.norm_last = self.fresh()
        for by in (1, 2, 3):
            to = self.norm_in.at[3 * k - 3 + by]
            self.copy(self.norm_src.at[k], to, self.peer(axis, by), self.norm_last, 5 + k)

    def end(self):
        self.norm_src[4] = self.norm_total(4)
        out = pltpu.make_async_copy(self.norm_src.at[4], self.norm, self.load_sem.at[4])
        out.start()
        for q in range(4):
            self.exchanged(self.pieces.at[0], self.shard.at[q], self.fin_recv.at[q])
        out.wait()


def kernel(*refs):
    body = Body(refs)
    body.run()
    assert body.used == RECEIVES and body.singles == SENDS, (body.used, body.singles)


def update(*refs):
    dx, *shard_in, dx_out, new_master, new_one, new_two = refs[:10]
    held, *held_in, put_master, put_one, put_two, into_sem, out_sem, small_in, small_out = refs[10:]
    parts = 4
    rows = [pl.ds(TOK // parts * i, TOK // parts) for i in range(parts)]
    into = [pltpu.make_async_copy(dx.at[rows[i]], held.at[i], into_sem.at[i]) for i in range(parts)]
    out = [pltpu.make_async_copy(held.at[i], dx_out.at[rows[i]], out_sem.at[i]) for i in range(parts)]
    loads = [pltpu.make_async_copy(a, b, small_in.at[i]) for i, (a, b) in enumerate(zip(shard_in, held_in))]
    for c in loads[:2] + into[:2] + loads[2:] + into[2:]:
        c.start()
    shard, norm, master, one, two = held_in
    for c in loads[:2] + into[:2]:
        c.wait()
    out[0].start()
    out[1].start()
    limit = jnp.sqrt(jnp.float32(DIN * DOUT))
    clip = jnp.minimum(1.0, limit / (jnp.sqrt(norm[0:1, 0:1]) + 1e-06))
    for c in loads[2:] + into[2:]:
        c.wait()
    out[2].start()
    out[3].start()
    for q in range(4):
        for j in range(CHUNKS):
            cols = slice(512 * j + 128 * q, 512 * j + 128 * (q + 1))
            clipped = shard[q, :, 128 * j : 128 * (j + 1)] * clip
            weight = master[:, cols]
            first = 0.9 * one[:, cols] + 0.1 * clipped
            second = 0.999 * two[:, cols] + 0.001 * clipped * clipped
            first_hat = first / (1.0 - 0.9**STEP)
            second_hat = second / (1.0 - 0.999**STEP)
            put_one[:, cols] = first
            put_two[:, cols] = second
            put_master[:, cols] = weight - 0.01 * (
                first_hat / (jnp.sqrt(second_hat) + 1e-08) + 0.1 * weight
            )
    for i, (a, b) in enumerate(((put_one, new_one), (put_two, new_two), (put_master, new_master))):
        c = pltpu.make_async_copy(a, b, small_out.at[i])
        c.start()
        out.append(c)
    for c in out:
        c.wait()


def on_device(attn_out, out_grad, master, moment_one, moment_two):
    anywhere = pl.BlockSpec(memory_space=pl.ANY)
    vmem = pl.BlockSpec(memory_space=pltpu.VMEM)
    dx, shard, norm = pl.pallas_call(
        kernel,
        out_shape=(
            jax.ShapeDtypeStruct((TOK, DIN), BF),
            jax.ShapeDtypeStruct((4, OWN, WIDE), F32),
            jax.ShapeDtypeStruct((8, 128), F32),
        ),
        in_specs=[anywhere] * 3,
        out_specs=(anywhere,) * 3,
        scratch_shapes=[
            pltpu.VMEM((2, TOK, HALF), BF),
            pltpu.VMEM((2, HALF, TOK), BF),
            pltpu.VMEM((2 * TOK, DOUT), BF),
            pltpu.VMEM((CHUNKS, HALF, 512), F32),
            pltpu.VMEM((CHUNKS, 2, 2, 4, 2, 2, ROWS, 128), BF),
            pltpu.VMEM((CHUNKS, 2, 2, 4, 2, 2, ROWS, 128), BF),
            pltpu.VMEM((CHUNKS, 3, ROWS, 128), BF),
            pltpu.VMEM((2 * TOK, HALF), F32),
            pltpu.VMEM((OWN, DOUT), F32),
            pltpu.VMEM((4, OWN, WIDE), BF),
            pltpu.VMEM((4, OWN, WIDE), BF),
            pltpu.VMEM((ROWS, WIDE), F32),
            pltpu.VMEM((ROWS, WIDE), F32),
            pltpu.VMEM((4, OWN, WIDE), F32),
            pltpu.VMEM((5, 8, 128), F32),
            pltpu.VMEM((10, 8, 128), F32),
            pltpu.SemaphoreType.DMA((8,)),
            pltpu.SemaphoreType.DMA((9,)),
            pltpu.SemaphoreType.DMA((SENDS,)),
            pltpu.SemaphoreType.DMA((RECEIVES,)),
            pltpu.SemaphoreType.DMA((4,)),
            pltpu.SemaphoreType.DMA((4,)),
            *(pltpu.VMEM(landing_shape(axes[:1]), BF) for axes in SCATTER),
            *(pltpu.VMEM(landing_shape(axes[:2]), BF) for axes in SCATTER),
        ],
        compiler_params=pltpu.CompilerParams(
            collective_id=0, has_side_effects=True, vmem_limit_bytes=66_000_000
        ),
        cost_estimate=pl.CostEstimate(
            flops=4 * TOK * DIN * DOUT, bytes_accessed=40_000_000, transcendentals=0
        ),
        name="step",
    )(attn_out, out_grad, master)
    part = jax.ShapeDtypeStruct((OWN, DOUT), F32)
    row = pltpu.VMEM((OWN, DOUT), F32)
    return pl.pallas_call(
        update,
        out_shape=(jax.ShapeDtypeStruct((TOK, DIN), BF), part, part, part),
        in_specs=[anywhere] * 6,
        out_specs=(anywhere,) * 4,
        scratch_shapes=[
            pltpu.VMEM((4, TOK // 4, DIN), BF),
            pltpu.VMEM((4, OWN, WIDE), F32),
            pltpu.VMEM((8, 128), F32),
            *(row,) * 6,
            pltpu.SemaphoreType.DMA((4,)),
            pltpu.SemaphoreType.DMA((4,)),
            pltpu.SemaphoreType.DMA((5,)),
            pltpu.SemaphoreType.DMA((3,)),
        ],
        name="update",
    )(dx, shard, norm, master, moment_one, moment_two)


def solution(mesh):
    split = P(("seq", "batch"), None)
    return jax.shard_map(
        on_device, mesh=mesh, in_specs=(split,) * 5, out_specs=(split,) * 4, check_vma=False
    )
```

```python
import jax
import jax.numpy as jnp
from jax import lax
from jax.experimental import pallas as pl
from jax.experimental.pallas import tpu as pltpu
from jax.sharding import PartitionSpec as P

DIN = 2560
DOUT = 2560
STEP = 10
TOK = 512
HALF = DIN // 2
ROWS = 80
CHUNKS = 5
OWN = 20
WIDE = 640
BF = jnp.bfloat16
F32 = jnp.float32
MESH = pl.DeviceIdType.MESH
RECEIVES = 84
SENDS = 19
AXES = ("y", "x", "z")
SPLITS = ("x", "z", "y")

GATHER = (("x", "y", "z"), ("y", "z", "x"), ("z", "y", "x"), ("x", "z", "y"), ("y", "z", "x"))
SCATTER = (("z", "y", "x"), ("x", "y", "z"), ("y", "z", "x"), ("z", "y", "x"), ("x", "z", "y"))

ORDER = (
    ("p1", 2), ("p1", 1), ("p1", 4), ("p1", 0), ("tr2",), ("rh", 0), ("pre",), ("ags", 3), ("ags", 1),
    ("rh", 2), ("ags", 2), ("rh", 1), ("p1", 3), ("rhm", 0), ("agm", 2), ("rhm", 1), ("rhm", 2), ("agm", 1),
    ("ags", 0), ("agm", 3), ("rm", 0), ("ags", 4), ("agmf", 1), ("rh", 3), ("rh", 4), ("agmf", 2), ("rmm", 0),
    ("rm", 1), ("agm", 0), ("agmf", 3), ("agh", 1), ("rhm", 3), ("rhm", 4), ("rm", 2), ("rmm", 1), ("rs", 0),
    ("agh", 3), ("rm", 4), ("agm", 4), ("agmf", 0), ("rm", 3), ("rmm", 2), ("aghf", 1), ("rmm", 4), ("aghf", 3),
    ("agmf", 4), ("rs", 1), ("agh", 2), ("rmm", 3), ("rs", 4), ("agh", 4), ("rs", 2), ("rs", 3), ("rz", 0),
    ("rz", 1), ("agh", 0), ("dx", 1), ("aghf", 2), ("rz", 2), ("rz", 3), ("rz", 4), ("fin",), ("n", 1),
    ("aghf", 4), ("aghf", 0), ("dx", 3), ("n", 2), ("dx", 2), ("dx", 4), ("n", 3), ("dx", 0), ("end",),
)


def where(chunk, chosen):
    every = pl.ds(0, 2)
    y_col, y_row = chosen.get("y", (every, every))
    z_col, z_row = chosen.get("z", (every, every))
    return (chunk, y_col, z_col, chosen.get("x", pl.ds(0, 4)), z_row, y_row)


DIMS = (("y", 0, 2), ("z", 0, 2), ("x", 0, 4), ("z", 1, 2), ("y", 1, 2))


def landing_shape(gone):
    return (3, *(size for axis, _, size in DIMS if axis not in gone), ROWS, 128)


def halves(axis):
    if axis == "x":
        return pl.ds(0, 2), pl.ds(2, 2)
    return (pl.ds(0, 2), pl.ds(0, 1)), (pl.ds(0, 2), pl.ds(1, 1))


class Body:
    def __init__(self, refs):
        (
            self.attn, self.og, self.master,
            self.dx, self.shard, self.norm,
            self.attn_v, self.attn_t, self.og_v, self.acc, self.grad, self.full, self.r_small, self.dx_acc,
            self.mst, self.give_w, self.stage, self.block, self.summed, self.pieces,
            self.norm_src, self.norm_in,
            self.load_sem, self.send, self.single, self.recv, self.pre_recv, self.fin_recv,
            *landings,
        ) = refs
        self.r_large, self.r_mid = landings[:CHUNKS], landings[CHUNKS:]
        self.used = 0
        self.singles = 0
        self.sent = []
        self.late = []
        self.live = {}
        seq = lax.axis_index("seq")
        batch = lax.axis_index("batch")
        self.zh = seq // 4
        self.core = batch % 2
        self.zl = batch // 8
        self.at = {"x": seq % 4, "y": (batch // 2) % 4, "z": self.zh * 2 + self.zl}

    def device(self, x, y, z, core):
        return ((z // 2) * 4 + x, ((z % 2) * 4 + y) * 2 + core)

    def shifted(self, axis, by):
        return (self.at[axis] + by) % 4

    def peer(self, axis, by):
        place = dict(self.at)
        place[axis] = self.shifted(axis, by)
        return self.device(place["x"], place["y"], place["z"], self.core)

    def partner(self):
        return self.device(self.at["x"], self.at["y"], self.at["z"], 1 - self.core)

    def place(self, axis, by=0):
        at = self.shifted(axis, by)
        if axis == "x":
            return at
        if axis == "y":
            return (at % 2, at // 2)
        turned = (at + 2 * self.core) % 4
        col = turned // 2
        return (col, turned + col * (3 - 2 * turned))

    def fresh(self):
        self.used += 1
        return self.used - 1

    def own_send(self):
        self.singles += 1
        return self.single.at[self.singles - 1]

    def copy(self, src, dst, device, recv=None, group=None):
        n = self.fresh() if recv is None else recv
        c = pltpu.make_async_remote_copy(
            src_ref=src, dst_ref=dst,
            send_sem=self.own_send() if group is None else self.send.at[group],
            recv_sem=self.recv.at[n], device_id=device, device_id_type=MESH,
        )
        c.start()
        if group is None:
            self.sent.append(c)
        return c

    def take(self, like, n):
        self.exchanged(like, like, self.recv.at[n])

    def drain(self):
        for group in range(9):
            blocks = self.full.at[:, :, :, pl.ds(0, 3)]
            if group % 3 == 1:
                blocks = self.full.at[:, pl.ds(0, 1), pl.ds(0, 1), pl.ds(0, 3)]
            if group % 3 == 2:
                one = pl.ds(0, 1)
                blocks = self.full.at[:, one, one, pl.ds(0, 3), one, one]
            if group > 5:
                blocks = self.norm_in.at[pl.ds(1, 3)]
            pltpu.make_async_remote_copy(
                src_ref=blocks, dst_ref=blocks, send_sem=self.send.at[group], recv_sem=self.recv.at[0],
                device_id=self.partner(), device_id_type=MESH,
            ).wait_send()

    def worker_place(self, q):
        z_col = q % 2
        turned = self.zl if z_col == 0 else 3 - self.zl
        return 2 * (self.at["y"] // 2) + q // 2, (turned + 2 * self.zh) % 4, self.zh

    def owner_place(self, i):
        z_row = self.place("z")[1]
        return 2 * (self.at["y"] // 2) + i // 2, 2 * self.core + z_row, i % 2

    def exchange(self, src, dst, recv, place):
        y, z, core = place
        away = pltpu.make_async_remote_copy(
            src_ref=src, dst_ref=dst, send_sem=self.own_send(), recv_sem=recv,
            device_id=self.device(self.at["x"], y, z, core), device_id_type=MESH,
        )
        here = pltpu.make_async_copy(src, dst, recv)
        mine = (y == self.at["y"]) & (z == self.at["z"]) & (core == self.core)
        pl.when(mine)(here.start)
        pl.when(jnp.logical_not(mine))(away.start)
        self.late.append((jnp.logical_not(mine), away))

    def exchanged(self, like, dst, recv):
        pltpu.make_async_remote_copy(
            src_ref=like, dst_ref=dst, send_sem=self.single.at[0], recv_sem=recv,
            device_id=self.partner(), device_id_type=MESH,
        ).wait_recv()

    def run(self):
        half = pl.multiple_of(self.core * HALF, 128)
        other = pl.multiple_of((1 - self.core) * HALF, 128)
        loads = [
            pltpu.make_async_copy(self.master, self.mst, self.load_sem.at[0]),
            pltpu.make_async_copy(self.attn.at[:, pl.ds(half, HALF)], self.attn_v.at[0], self.load_sem.at[1]),
            pltpu.make_async_copy(self.og, self.og_v.at[pl.ds(0, TOK)], self.load_sem.at[2]),
        ]
        for load in loads:
            load.start()
        barrier = pltpu.get_barrier_semaphore()
        greeted = [self.partner()]
        for axis in AXES:
            greeted += [self.peer(axis, by) for by in (1, 2, 3)]
        for q in range(4):
            for place in (self.worker_place(q), self.owner_place(q)):
                greeted.append(self.device(self.at["x"], *place))
        for device in greeted:
            pl.semaphore_signal(barrier, inc=1, device_id=device, device_id_type=MESH)
        loads[0].wait()
        for q in range(4):
            self.give_w[q] = jnp.concatenate(
                [self.mst[:, 512 * j + 128 * q : 512 * j + 128 * (q + 1)] for j in range(CHUNKS)], axis=1
            ).astype(BF)
        loads[1].wait()
        self.transpose(0)
        pl.semaphore_wait(barrier, len(greeted))

        part = HALF // 2
        self.swap_attn = [
            self.copy(
                self.attn.at[:, pl.ds(pl.multiple_of(other + part * i, 128), part)],
                self.attn_v.at[1, :, pl.ds(part * i, part)],
                self.partner(),
            )
            for i in range(2)
        ]
        slot = (self.at["y"] % 2) * 2 + self.core
        for q in range(4):
            self.exchange(
                self.give_w.at[q], self.stage.at[slot], self.pre_recv.at[slot], self.worker_place(q)
            )
        self.swap_og = [
            self.copy(
                self.og.at[:, pl.ds(512 * j, 512)], self.og_v.at[pl.ds(TOK, TOK), pl.ds(512 * j, 512)],
                self.partner(),
            )
            for j in range(CHUNKS)
        ]
        loads[2].wait()

        sums = [step for step in ORDER if step[0] == "dx"]
        for step in ORDER:
            name = step[0]
            if step == sums[0]:
                name = "dx_first"
            elif step == sums[-1]:
                name = "dx_last"
            elif step in sums:
                name = "dx_more"
            getattr(self, name)(*step[1:])

        self.drain()
        for c in self.sent:
            c.wait_send()
        for go, c in self.late:
            pl.when(go)(c.wait_send)

    def transpose(self, which, first=0, last=10):
        def body(i, carry):
            lanes = pl.ds(pl.multiple_of(i * 128, 128), 128)
            self.attn_t[which, lanes, :] = self.attn_v[which, :, lanes].T
            return carry

        lax.fori_loop(first, last, body, 0)

    def tr2(self):
        for i in range(2):
            self.swap_attn[i].wait_recv()
            self.transpose(1, 5 * i, 5 * i + 5)

    def p1(self, j):
        self.acc[j] = jnp.dot(
            self.attn_t[0], self.og_v[pl.ds(0, TOK), pl.ds(512 * j, 512)], preferred_element_type=F32
        )

    def pre(self):
        for s in range(4):
            self.exchanged(self.give_w.at[0], self.stage.at[s], self.pre_recv.at[s])
            self.block[OWN * s : OWN * (s + 1), :] = self.stage[s].astype(F32)
        here = {axis: self.place(axis) for axis in AXES}
        for j in range(CHUNKS):
            self.full[where(j, here)] = self.block[:, 128 * j : 128 * (j + 1)].astype(BF)

    def ags(self, j):
        axis = GATHER[j][2]
        here = self.full.at[where(j, {a: self.place(a) for a in AXES})]
        n = self.fresh()
        for by in (1, 3, 2):
            self.copy(here, here, self.peer(axis, by), n, 2)
        self.live["ags", j] = (n, self.r_small.at[j])

    def ring(self, j, axis, fixed, key, group, both):
        chosen = {a: self.place(a) for a in fixed}
        split = next(a for a in SPLITS if a != axis and a not in chosen)
        first, second = halves(split)

        def part(by, rows):
            return self.full.at[where(j, {**chosen, axis: self.place(axis, by), split: rows})]

        ahead, behind = self.peer(axis, 1), self.peer(axis, 3)
        n = self.fresh()
        top_ahead = self.copy(part(0, first), part(0, first), ahead, None, group)
        low_behind = self.copy(part(0, second), part(0, second), behind, None, group)
        self.copy(part(0, second), part(0, second), ahead, n, group)
        self.copy(part(0, first), part(0, first), behind, n, group)
        self.live[key] = (top_ahead, low_behind, part, first, second, n, group, both)

    def forward(self, axis, key):
        top_ahead, low_behind, part, first, second, n, group, both = self.live[key]
        top_ahead.wait_recv()
        self.copy(part(3, first), part(3, first), self.peer(axis, 1), n, group)
        low_behind.wait_recv()
        self.copy(part(1, second), part(1, second), self.peer(axis, 3), n, group)
        self.live[key] = (n, both)

    def finish(self, key):
        n, like = self.live[key]
        self.take(like, n)

    def agm(self, j):
        self.finish(("ags", j))
        self.ring(j, GATHER[j][1], (GATHER[j][0],), ("agm", j), 1, self.r_mid[j].at[pl.ds(0, 2)])

    def agmf(self, j):
        self.forward(GATHER[j][1], ("agm", j))

    def agh(self, j):
        self.finish(("agm", j))
        self.ring(j, GATHER[j][0], (), ("agh", j), 0, self.r_large[j].at[pl.ds(0, 2)])

    def aghf(self, j):
        self.forward(GATHER[j][0], ("agh", j))

    def dx_dot(self, j, rows, first=0, last=HALF):
        left = self.og_v[rows, pl.ds(512 * j, 512)]
        right = jnp.concatenate(
            [self.full[j, q // 2, q % 2].reshape(HALF, 128)[first:last] for q in range(4)], axis=1
        )
        return lax.dot_general(left, right, (((1,), (1,)), ((), ())), preferred_element_type=F32)

    def dx_first(self, j):
        self.finish(("agh", j))
        self.dx_acc[...] = self.dx_dot(j, pl.ds(0, 2 * TOK))

    def dx_more(self, j):
        self.finish(("agh", j))
        self.dx_acc[...] += self.dx_dot(j, pl.ds(0, 2 * TOK))

    def dx_last(self, j):
        self.finish(("agh", j))
        start = self.core * HALF
        gives, keeps = [], []
        for which, rows in ((1, pl.ds(TOK, TOK)), (0, pl.ds(0, TOK))):
            for i, (first, last) in enumerate(((0, 512), (512, 1024), (1024, HALF))):
                cols = pl.ds(first, last - first)
                done = self.dx_acc[rows, cols] + self.dx_dot(j, rows, first, last)
                self.attn_v[which, :, cols] = done.astype(BF)
                src = self.attn_v.at[which, :, cols]
                to = self.dx.at[:, pl.ds(pl.multiple_of(start + first, 128), last - first)]
                if which:
                    gives.append(self.copy(src, to, self.partner()))
                else:
                    keep = pltpu.make_async_copy(src, to, self.load_sem.at[5 + i])
                    keep.start()
                    keeps.append(keep)
        for c in gives:
            c.wait_recv()
        for c in keeps:
            c.wait()

    def rh(self, j):
        self.swap_og[j].wait_recv()
        v = self.acc[j] + jnp.dot(
            self.attn_t[1], self.og_v[pl.ds(TOK, TOK), pl.ds(512 * j, 512)], preferred_element_type=F32
        )
        v = v.astype(BF)
        for q in range(4):
            self.grad[j, q // 2, q % 2] = v[:, 128 * q : 128 * (q + 1)].reshape(4, 2, 2, ROWS, 128)
        self.reduce(j, SCATTER[j][0], (), self.r_large[j], ("rh", j), 3)

    def reduce(self, j, axis, fixed, landing, key, group):
        chosen = {a: self.place(a) for a in fixed}
        split = next(a for a in SPLITS if a != axis and a not in chosen)
        first, second = halves(split)
        ahead, behind = self.peer(axis, 1), self.peer(axis, 3)

        def part(by, rows):
            return where(j, {**chosen, axis: self.place(axis, by), split: rows})

        def land(slot, rows):
            index = [slot]
            for a, k, size in DIMS:
                if a == split:
                    index.append(rows if a == "x" else rows[k])
                elif a != axis and a not in chosen:
                    index.append(pl.ds(0, size))
            return tuple(index)

        n = self.fresh()

        def send(by, rows, slot, device, recv):
            return self.copy(
                self.grad.at[part(by, rows)], landing.at[land(slot, rows)], device, recv, group
            )

        far_ahead = send(2, first, 0, ahead, None)
        far_behind = send(2, second, 0, behind, None)
        send(1, second, 1, ahead, n)
        send(3, first, 2, behind, n)
        self.live[key] = (far_ahead, far_behind, part, land, first, second, n, send)

    def pass_on(self, axis, landing, key):
        far_ahead, far_behind, part, land, first, second, n, send = self.live[key]
        far_ahead.wait_recv()
        at = part(1, first)
        self.grad[at] = (self.grad[at].astype(F32) + landing[land(0, first)].astype(F32)).astype(BF)
        send(1, first, 1, self.peer(axis, 1), n)
        far_behind.wait_recv()
        at = part(3, second)
        self.grad[at] = (self.grad[at].astype(F32) + landing[land(0, second)].astype(F32)).astype(BF)
        send(3, second, 2, self.peer(axis, 3), n)
        self.live[key] = (n, landing.at[pl.ds(0, 2)])

    def rhm(self, j):
        self.pass_on(SCATTER[j][0], self.r_large[j], ("rh", j))

    def rm(self, j):
        self.finish(("rh", j))
        large, mid, small = SCATTER[j]
        at = where(j, {large: self.place(large)})
        landed = self.r_large[j]
        total = self.grad[at].astype(F32) + landed[1].astype(F32)
        self.grad[at] = (total + landed[2].astype(F32)).astype(BF)
        self.reduce(j, mid, (large,), self.r_mid[j], ("rm", j), 4)

    def rmm(self, j):
        self.pass_on(SCATTER[j][1], self.r_mid[j], ("rm", j))

    def rs(self, j):
        self.finish(("rm", j))
        large, mid, small = SCATTER[j]
        chosen = {large: self.place(large), mid: self.place(mid)}
        at = where(j, chosen)
        landed = self.r_mid[j]
        total = self.grad[at].astype(F32) + landed[1].astype(F32)
        self.grad[at] = (total + landed[2].astype(F32)).astype(BF)
        n = self.fresh()
        for by in (1, 3, 2):
            at = where(j, {**chosen, small: self.place(small, by)})
            self.copy(self.grad.at[at], self.r_small.at[j, by - 1], self.peer(small, by), n, 5)
        self.live["rs", j] = (n, self.r_small.at[j])

    def rz(self, j):
        self.finish(("rs", j))
        total = self.grad[where(j, {a: self.place(a) for a in AXES})].astype(F32)
        for s in range(3):
            total += self.r_small[j, s].astype(F32)
        self.summed[:, 128 * j : 128 * (j + 1)] = total

    def fin(self):
        total = self.summed[...]
        squares = jnp.sum(total * total, axis=(0, 1), keepdims=True)
        self.norm_src[0] = jnp.broadcast_to(squares, (8, 128))
        self.norm_last = self.fresh()
        self.copy(self.norm_src.at[0], self.norm_in.at[0], self.partner(), self.norm_last)
        piece = self.place("y")[0] * 2 + self.place("z")[0]
        for i in range(4):
            self.pieces[i] = self.summed[OWN * i : OWN * (i + 1), :]
            self.exchange(
                self.pieces.at[i], self.shard.at[piece], self.fin_recv.at[piece], self.owner_place(i)
            )

    def norm_total(self, k):
        total = self.norm_src[k - 1]
        first, count = (0, 1) if k == 1 else (3 * k - 5, 3)
        self.take(self.norm_in.at[pl.ds(first, count)], self.norm_last)
        for s in range(count):
            total += self.norm_in[first + s]
        return total

    def n(self, k):
        self.norm_src[k] = self.norm_total(k)
        axis = AXES[k - 1]
        self.norm_last = self.fresh()
        for by in (1, 2, 3):
            to = self.norm_in.at[3 * k - 3 + by]
            self.copy(self.norm_src.at[k], to, self.peer(axis, by), self.norm_last, 5 + k)

    def end(self):
        self.norm_src[4] = self.norm_total(4)
        out = pltpu.make_async_copy(self.norm_src.at[4], self.norm, self.load_sem.at[4])
        out.start()
        for q in range(4):
            self.exchanged(self.pieces.at[0], self.shard.at[q], self.fin_recv.at[q])
        out.wait()


def kernel(*refs):
    body = Body(refs)
    body.run()
    assert body.used == RECEIVES and body.singles == SENDS, (body.used, body.singles)


def update(*refs):
    dx, *shard_in, dx_out, new_master, new_one, new_two = refs[:10]
    held, *held_in, put_master, put_one, put_two, into_sem, out_sem, small_in, small_out = refs[10:]
    parts = 8
    rows = [pl.ds(TOK // parts * i, TOK // parts) for i in range(parts)]
    into = [pltpu.make_async_copy(dx.at[rows[i]], held.at[i], into_sem.at[i]) for i in range(parts)]
    out = [pltpu.make_async_copy(held.at[i], dx_out.at[rows[i]], out_sem.at[i]) for i in range(parts)]
    loads = [pltpu.make_async_copy(a, b, small_in.at[i]) for i, (a, b) in enumerate(zip(shard_in, held_in))]
    for c in loads[:2] + into[:4] + loads[2:] + into[4:]:
        c.start()
    shard, norm, master, one, two = held_in
    for c in loads[:2]:
        c.wait()
    for i in range(4):
        into[i].wait()
        out[i].start()
    limit = jnp.sqrt(jnp.float32(DIN * DOUT))
    clip = jnp.minimum(1.0, limit / (jnp.sqrt(norm[0:1, 0:1]) + 1e-06))
    for i in range(4, parts):
        into[i].wait()
        out[i].start()
    for c in loads[2:]:
        c.wait()
    for q in range(4):
        for j in range(CHUNKS):
            cols = slice(512 * j + 128 * q, 512 * j + 128 * (q + 1))
            clipped = shard[q, :, 128 * j : 128 * (j + 1)] * clip
            weight = master[:, cols]
            first = 0.9 * one[:, cols] + 0.1 * clipped
            second = 0.999 * two[:, cols] + 0.001 * clipped * clipped
            first_hat = first / (1.0 - 0.9**STEP)
            second_hat = second / (1.0 - 0.999**STEP)
            put_one[:, cols] = first
            put_two[:, cols] = second
            put_master[:, cols] = weight - 0.01 * (
                first_hat / (jnp.sqrt(second_hat) + 1e-08) + 0.1 * weight
            )
    for i, (a, b) in enumerate(((put_one, new_one), (put_two, new_two), (put_master, new_master))):
        c = pltpu.make_async_copy(a, b, small_out.at[i])
        c.start()
        out.append(c)
    for c in out:
        c.wait()


def on_device(attn_out, out_grad, master, moment_one, moment_two):
    anywhere = pl.BlockSpec(memory_space=pl.ANY)
    vmem = pl.BlockSpec(memory_space=pltpu.VMEM)
    dx, shard, norm = pl.pallas_call(
        kernel,
        out_shape=(
            jax.ShapeDtypeStruct((TOK, DIN), BF),
            jax.ShapeDtypeStruct((4, OWN, WIDE), F32),
            jax.ShapeDtypeStruct((8, 128), F32),
        ),
        in_specs=[anywhere] * 3,
        out_specs=(anywhere,) * 3,
        scratch_shapes=[
            pltpu.VMEM((2, TOK, HALF), BF),
            pltpu.VMEM((2, HALF, TOK), BF),
            pltpu.VMEM((2 * TOK, DOUT), BF),
            pltpu.VMEM((CHUNKS, HALF, 512), F32),
            pltpu.VMEM((CHUNKS, 2, 2, 4, 2, 2, ROWS, 128), BF),
            pltpu.VMEM((CHUNKS, 2, 2, 4, 2, 2, ROWS, 128), BF),
            pltpu.VMEM((CHUNKS, 3, ROWS, 128), BF),
            pltpu.VMEM((2 * TOK, HALF), F32),
            pltpu.VMEM((OWN, DOUT), F32),
            pltpu.VMEM((4, OWN, WIDE), BF),
            pltpu.VMEM((4, OWN, WIDE), BF),
            pltpu.VMEM((ROWS, WIDE), F32),
            pltpu.VMEM((ROWS, WIDE), F32),
            pltpu.VMEM((4, OWN, WIDE), F32),
            pltpu.VMEM((5, 8, 128), F32),
            pltpu.VMEM((10, 8, 128), F32),
            pltpu.SemaphoreType.DMA((8,)),
            pltpu.SemaphoreType.DMA((9,)),
            pltpu.SemaphoreType.DMA((SENDS,)),
            pltpu.SemaphoreType.DMA((RECEIVES,)),
            pltpu.SemaphoreType.DMA((4,)),
            pltpu.SemaphoreType.DMA((4,)),
            *(pltpu.VMEM(landing_shape(axes[:1]), BF) for axes in SCATTER),
            *(pltpu.VMEM(landing_shape(axes[:2]), BF) for axes in SCATTER),
        ],
        compiler_params=pltpu.CompilerParams(
            collective_id=0, has_side_effects=True, vmem_limit_bytes=66_000_000
        ),
        cost_estimate=pl.CostEstimate(
            flops=4 * TOK * DIN * DOUT, bytes_accessed=40_000_000, transcendentals=0
        ),
        name="step",
    )(attn_out, out_grad, master)
    part = jax.ShapeDtypeStruct((OWN, DOUT), F32)
    row = pltpu.VMEM((OWN, DOUT), F32)
    return pl.pallas_call(
        update,
        out_shape=(jax.ShapeDtypeStruct((TOK, DIN), BF), part, part, part),
        in_specs=[anywhere] * 6,
        out_specs=(anywhere,) * 4,
        scratch_shapes=[
            pltpu.VMEM((8, TOK // 8, DIN), BF),
            pltpu.VMEM((4, OWN, WIDE), F32),
            pltpu.VMEM((8, 128), F32),
            *(row,) * 6,
            pltpu.SemaphoreType.DMA((8,)),
            pltpu.SemaphoreType.DMA((8,)),
            pltpu.SemaphoreType.DMA((5,)),
            pltpu.SemaphoreType.DMA((3,)),
        ],
        name="update",
    )(dx, shard, norm, master, moment_one, moment_two)


def solution(mesh):
    split = P(("seq", "batch"), None)
    return jax.shard_map(
        on_device, mesh=mesh, in_specs=(split,) * 5, out_specs=(split,) * 4, check_vma=False
    )
```

```python
import jax
import jax.numpy as jnp
from jax import lax
from jax.experimental import pallas as pl
from jax.experimental.pallas import tpu as pltpu
from jax.sharding import PartitionSpec as P

DIN = 2560
DOUT = 2560
STEP = 10
TOK = 512
HALF = DIN // 2
ROWS = 80
CHUNKS = 5
OWN = 20
WIDE = 640
BF = jnp.bfloat16
F32 = jnp.float32
MESH = pl.DeviceIdType.MESH
RECEIVES = 83
SENDS = 25
AXES = ("y", "x", "z")
SPLITS = ("x", "z", "y")

GATHER = (("x", "y", "z"), ("y", "z", "x"), ("z", "y", "x"), ("x", "z", "y"), ("y", "z", "x"))
SCATTER = (("z", "y", "x"), ("x", "y", "z"), ("y", "z", "x"), ("z", "y", "x"), ("x", "z", "y"))

ORDER = (
    ("p1", 2), ("p1", 1), ("p1", 4), ("p1", 0), ("tr2",), ("rh", 0), ("pre",), ("ags", 3), ("ags", 1),
    ("rh", 2), ("ags", 2), ("rh", 1), ("p1", 3), ("rhm", 0), ("agm", 2), ("rhm", 1), ("rhm", 2), ("agm", 1),
    ("ags", 0), ("agm", 3), ("rm", 0), ("ags", 4), ("agmf", 1), ("rh", 3), ("rh", 4), ("agmf", 2), ("rmm", 0),
    ("rm", 1), ("agm", 0), ("agmf", 3), ("agh", 1), ("rhm", 3), ("rhm", 4), ("rm", 2), ("rmm", 1), ("rs", 0),
    ("agh", 3), ("rm", 4), ("agm", 4), ("agmf", 0), ("rm", 3), ("rmm", 2), ("aghf", 1), ("rmm", 4), ("aghf", 3),
    ("agmf", 4), ("rs", 1), ("agh", 2), ("rmm", 3), ("rs", 4), ("agh", 4), ("rs", 2), ("rs", 3), ("rz", 0),
    ("rz", 1), ("agh", 0), ("dx", 1), ("aghf", 2), ("rz", 2), ("rz", 3), ("rz", 4), ("fin",), ("aghf", 4),
    ("aghf", 0), ("dx", 3), ("n", 1), ("dx", 2), ("dx", 4), ("n", 2), ("dx", 0), ("end",),
)


def where(chunk, chosen):
    every = pl.ds(0, 2)
    y_col, y_row = chosen.get("y", (every, every))
    z_col, z_row = chosen.get("z", (every, every))
    return (chunk, y_col, z_col, chosen.get("x", pl.ds(0, 4)), z_row, y_row)


DIMS = (("y", 0, 2), ("z", 0, 2), ("x", 0, 4), ("z", 1, 2), ("y", 1, 2))


def landing_shape(gone):
    return (3, *(size for axis, _, size in DIMS if axis not in gone), ROWS, 128)


def halves(axis):
    if axis == "x":
        return pl.ds(0, 2), pl.ds(2, 2)
    return (pl.ds(0, 2), pl.ds(0, 1)), (pl.ds(0, 2), pl.ds(1, 1))


class Body:
    def __init__(self, refs):
        (
            self.attn, self.og, self.master,
            self.dx, self.shard, self.norm,
            self.attn_v, self.attn_t, self.og_v, self.acc, self.grad, self.full, self.r_small, self.dx_acc,
            self.mst, self.give_w, self.stage, self.block, self.summed, self.pieces,
            self.norm_src, self.norm_in,
            self.load_sem, self.send, self.single, self.recv, self.pre_recv, self.fin_recv,
            *landings,
        ) = refs
        self.r_large, self.r_mid = landings[:CHUNKS], landings[CHUNKS:]
        self.used = 0
        self.singles = 0
        self.sent = []
        self.late = []
        self.live = {}
        seq = lax.axis_index("seq")
        batch = lax.axis_index("batch")
        self.zh = seq // 4
        self.core = batch % 2
        self.zl = batch // 8
        self.at = {"x": seq % 4, "y": (batch // 2) % 4, "z": self.zh * 2 + self.zl}

    def device(self, x, y, z, core):
        return ((z // 2) * 4 + x, ((z % 2) * 4 + y) * 2 + core)

    def shifted(self, axis, by):
        return (self.at[axis] + by) % 4

    def peer(self, axis, by):
        place = dict(self.at)
        place[axis] = self.shifted(axis, by)
        return self.device(place["x"], place["y"], place["z"], self.core)

    def across(self, by):
        return self.device(self.at["x"], self.shifted("y", by), self.at["z"], 1 - self.core)

    def partner(self):
        return self.device(self.at["x"], self.at["y"], self.at["z"], 1 - self.core)

    def place(self, axis, by=0):
        at = self.shifted(axis, by)
        if axis == "x":
            return at
        if axis == "y":
            return (at % 2, at // 2)
        turned = (at + 2 * self.core) % 4
        col = turned // 2
        return (col, turned + col * (3 - 2 * turned))

    def fresh(self):
        self.used += 1
        return self.used - 1

    def own_send(self):
        self.singles += 1
        return self.single.at[self.singles - 1]

    def copy(self, src, dst, device, recv=None, group=None):
        n = self.fresh() if recv is None else recv
        c = pltpu.make_async_remote_copy(
            src_ref=src, dst_ref=dst,
            send_sem=self.own_send() if group is None else self.send.at[group],
            recv_sem=self.recv.at[n], device_id=device, device_id_type=MESH,
        )
        c.start()
        if group is None:
            self.sent.append(c)
        return c

    def take(self, like, n):
        self.exchanged(like, like, self.recv.at[n])

    def drain(self):
        for group in range(8):
            blocks = self.full.at[:, :, :, pl.ds(0, 3)]
            if group % 3 == 1:
                blocks = self.full.at[:, pl.ds(0, 1), pl.ds(0, 1), pl.ds(0, 3)]
            if group % 3 == 2:
                one = pl.ds(0, 1)
                blocks = self.full.at[:, one, one, pl.ds(0, 3), one, one]
            if group > 5:
                blocks = self.norm_in.at[pl.ds(1, 3)]
            pltpu.make_async_remote_copy(
                src_ref=blocks, dst_ref=blocks, send_sem=self.send.at[group], recv_sem=self.recv.at[0],
                device_id=self.partner(), device_id_type=MESH,
            ).wait_send()

    def worker_place(self, q):
        z_col = q % 2
        turned = self.zl if z_col == 0 else 3 - self.zl
        return 2 * (self.at["y"] // 2) + q // 2, (turned + 2 * self.zh) % 4, self.zh

    def owner_place(self, i):
        z_row = self.place("z")[1]
        return 2 * (self.at["y"] // 2) + i // 2, 2 * self.core + z_row, i % 2

    def exchange(self, src, dst, recv, place):
        y, z, core = place
        away = pltpu.make_async_remote_copy(
            src_ref=src, dst_ref=dst, send_sem=self.own_send(), recv_sem=recv,
            device_id=self.device(self.at["x"], y, z, core), device_id_type=MESH,
        )
        here = pltpu.make_async_copy(src, dst, recv)
        mine = (y == self.at["y"]) & (z == self.at["z"]) & (core == self.core)
        pl.when(mine)(here.start)
        pl.when(jnp.logical_not(mine))(away.start)
        self.late.append((jnp.logical_not(mine), away))

    def exchanged(self, like, dst, recv):
        pltpu.make_async_remote_copy(
            src_ref=like, dst_ref=dst, send_sem=self.single.at[0], recv_sem=recv,
            device_id=self.partner(), device_id_type=MESH,
        ).wait_recv()

    def run(self):
        half = pl.multiple_of(self.core * HALF, 128)
        other = pl.multiple_of((1 - self.core) * HALF, 128)
        loads = [
            pltpu.make_async_copy(self.master, self.mst, self.load_sem.at[0]),
            pltpu.make_async_copy(self.attn.at[:, pl.ds(half, HALF)], self.attn_v.at[0], self.load_sem.at[1]),
            pltpu.make_async_copy(self.og, self.og_v.at[pl.ds(0, TOK)], self.load_sem.at[2]),
        ]
        for load in loads:
            load.start()
        barrier = pltpu.get_barrier_semaphore()
        greeted = [self.partner()] + [self.across(by) for by in (1, 2, 3)]
        for axis in AXES:
            greeted += [self.peer(axis, by) for by in (1, 2, 3)]
        for q in range(4):
            for place in (self.worker_place(q), self.owner_place(q)):
                greeted.append(self.device(self.at["x"], *place))
        for device in greeted:
            pl.semaphore_signal(barrier, inc=1, device_id=device, device_id_type=MESH)
        loads[0].wait()
        for q in range(4):
            self.give_w[q] = jnp.concatenate(
                [self.mst[:, 512 * j + 128 * q : 512 * j + 128 * (q + 1)] for j in range(CHUNKS)], axis=1
            ).astype(BF)
        loads[1].wait()
        self.transpose(0)
        pl.semaphore_wait(barrier, len(greeted))

        part = HALF // 2
        self.swap_attn = [
            self.copy(
                self.attn.at[:, pl.ds(pl.multiple_of(other + part * i, 128), part)],
                self.attn_v.at[1, :, pl.ds(part * i, part)],
                self.partner(),
            )
            for i in range(2)
        ]
        slot = (self.at["y"] % 2) * 2 + self.core
        for q in range(4):
            self.exchange(
                self.give_w.at[q], self.stage.at[slot], self.pre_recv.at[slot], self.worker_place(q)
            )
        self.swap_og = [
            self.copy(
                self.og.at[:, pl.ds(512 * j, 512)], self.og_v.at[pl.ds(TOK, TOK), pl.ds(512 * j, 512)],
                self.partner(),
            )
            for j in range(CHUNKS)
        ]
        loads[2].wait()

        sums = [step for step in ORDER if step[0] == "dx"]
        for step in ORDER:
            name = step[0]
            if step == sums[0]:
                name = "dx_first"
            elif step == sums[-1]:
                name = "dx_last"
            elif step in sums:
                name = "dx_more"
            getattr(self, name)(*step[1:])

        self.drain()
        for c in self.sent:
            c.wait_send()
        for go, c in self.late:
            pl.when(go)(c.wait_send)

    def transpose(self, which, first=0, last=10):
        def body(i, carry):
            lanes = pl.ds(pl.multiple_of(i * 128, 128), 128)
            self.attn_t[which, lanes, :] = self.attn_v[which, :, lanes].T
            return carry

        lax.fori_loop(first, last, body, 0)

    def tr2(self):
        for i in range(2):
            self.swap_attn[i].wait_recv()
            self.transpose(1, 5 * i, 5 * i + 5)

    def p1(self, j):
        self.acc[j] = jnp.dot(
            self.attn_t[0], self.og_v[pl.ds(0, TOK), pl.ds(512 * j, 512)], preferred_element_type=F32
        )

    def pre(self):
        for s in range(4):
            self.exchanged(self.give_w.at[0], self.stage.at[s], self.pre_recv.at[s])
            self.block[OWN * s : OWN * (s + 1), :] = self.stage[s].astype(F32)
        here = {axis: self.place(axis) for axis in AXES}
        for j in range(CHUNKS):
            self.full[where(j, here)] = self.block[:, 128 * j : 128 * (j + 1)].astype(BF)

    def ags(self, j):
        axis = GATHER[j][2]
        here = self.full.at[where(j, {a: self.place(a) for a in AXES})]
        n = self.fresh()
        for by in (1, 3, 2):
            self.copy(here, here, self.peer(axis, by), n, 2)
        self.live["ags", j] = (n, self.r_small.at[j])

    def ring(self, j, axis, fixed, key, group, both):
        chosen = {a: self.place(a) for a in fixed}
        split = next(a for a in SPLITS if a != axis and a not in chosen)
        first, second = halves(split)

        def part(by, rows):
            return self.full.at[where(j, {**chosen, axis: self.place(axis, by), split: rows})]

        ahead, behind = self.peer(axis, 1), self.peer(axis, 3)
        n = self.fresh()
        top_ahead = self.copy(part(0, first), part(0, first), ahead, None, group)
        low_behind = self.copy(part(0, second), part(0, second), behind, None, group)
        self.copy(part(0, second), part(0, second), ahead, n, group)
        self.copy(part(0, first), part(0, first), behind, n, group)
        self.live[key] = (top_ahead, low_behind, part, first, second, n, group, both)

    def forward(self, axis, key):
        top_ahead, low_behind, part, first, second, n, group, both = self.live[key]
        top_ahead.wait_recv()
        self.copy(part(3, first), part(3, first), self.peer(axis, 1), n, group)
        low_behind.wait_recv()
        self.copy(part(1, second), part(1, second), self.peer(axis, 3), n, group)
        self.live[key] = (n, both)

    def finish(self, key):
        n, like = self.live[key]
        self.take(like, n)

    def agm(self, j):
        self.finish(("ags", j))
        self.ring(j, GATHER[j][1], (GATHER[j][0],), ("agm", j), 1, self.r_mid[j].at[pl.ds(0, 2)])

    def agmf(self, j):
        self.forward(GATHER[j][1], ("agm", j))

    def agh(self, j):
        self.finish(("agm", j))
        self.ring(j, GATHER[j][0], (), ("agh", j), 0, self.r_large[j].at[pl.ds(0, 2)])

    def aghf(self, j):
        self.forward(GATHER[j][0], ("agh", j))

    def dx_dot(self, j, rows, first=0, last=HALF):
        left = self.og_v[rows, pl.ds(512 * j, 512)]
        right = jnp.concatenate(
            [self.full[j, q // 2, q % 2].reshape(HALF, 128)[first:last] for q in range(4)], axis=1
        )
        return lax.dot_general(left, right, (((1,), (1,)), ((), ())), preferred_element_type=F32)

    def dx_first(self, j):
        self.finish(("agh", j))
        self.dx_acc[...] = self.dx_dot(j, pl.ds(0, 2 * TOK))

    def dx_more(self, j):
        self.finish(("agh", j))
        self.dx_acc[...] += self.dx_dot(j, pl.ds(0, 2 * TOK))

    def dx_last(self, j):
        self.finish(("agh", j))
        start = self.core * HALF
        gives, keeps = [], []
        for which, rows in ((1, pl.ds(TOK, TOK)), (0, pl.ds(0, TOK))):
            for i, (first, last) in enumerate(((0, 512), (512, 1024), (1024, HALF))):
                cols = pl.ds(first, last - first)
                done = self.dx_acc[rows, cols] + self.dx_dot(j, rows, first, last)
                self.attn_v[which, :, cols] = done.astype(BF)
                src = self.attn_v.at[which, :, cols]
                to = self.dx.at[:, pl.ds(pl.multiple_of(start + first, 128), last - first)]
                if which:
                    gives.append(self.copy(src, to, self.partner()))
                else:
                    keep = pltpu.make_async_copy(src, to, self.load_sem.at[5 + i])
                    keep.start()
                    keeps.append(keep)
        for c in gives:
            c.wait_recv()
        for c in keeps:
            c.wait()

    def rh(self, j):
        self.swap_og[j].wait_recv()
        v = self.acc[j] + jnp.dot(
            self.attn_t[1], self.og_v[pl.ds(TOK, TOK), pl.ds(512 * j, 512)], preferred_element_type=F32
        )
        v = v.astype(BF)
        for q in range(4):
            self.grad[j, q // 2, q % 2] = v[:, 128 * q : 128 * (q + 1)].reshape(4, 2, 2, ROWS, 128)
        self.reduce(j, SCATTER[j][0], (), self.r_large[j], ("rh", j), 3)

    def reduce(self, j, axis, fixed, landing, key, group):
        chosen = {a: self.place(a) for a in fixed}
        split = next(a for a in SPLITS if a != axis and a not in chosen)
        first, second = halves(split)
        ahead, behind = self.peer(axis, 1), self.peer(axis, 3)

        def part(by, rows):
            return where(j, {**chosen, axis: self.place(axis, by), split: rows})

        def land(slot, rows):
            index = [slot]
            for a, k, size in DIMS:
                if a == split:
                    index.append(rows if a == "x" else rows[k])
                elif a != axis and a not in chosen:
                    index.append(pl.ds(0, size))
            return tuple(index)

        n = self.fresh()

        def send(by, rows, slot, device, recv):
            return self.copy(
                self.grad.at[part(by, rows)], landing.at[land(slot, rows)], device, recv, group
            )

        far_ahead = send(2, first, 0, ahead, None)
        far_behind = send(2, second, 0, behind, None)
        send(1, second, 1, ahead, n)
        send(3, first, 2, behind, n)
        self.live[key] = (far_ahead, far_behind, part, land, first, second, n, send)

    def pass_on(self, axis, landing, key):
        far_ahead, far_behind, part, land, first, second, n, send = self.live[key]
        far_ahead.wait_recv()
        at = part(1, first)
        self.grad[at] = (self.grad[at].astype(F32) + landing[land(0, first)].astype(F32)).astype(BF)
        send(1, first, 1, self.peer(axis, 1), n)
        far_behind.wait_recv()
        at = part(3, second)
        self.grad[at] = (self.grad[at].astype(F32) + landing[land(0, second)].astype(F32)).astype(BF)
        send(3, second, 2, self.peer(axis, 3), n)
        self.live[key] = (n, landing.at[pl.ds(0, 2)])

    def rhm(self, j):
        self.pass_on(SCATTER[j][0], self.r_large[j], ("rh", j))

    def rm(self, j):
        self.finish(("rh", j))
        large, mid, small = SCATTER[j]
        at = where(j, {large: self.place(large)})
        landed = self.r_large[j]
        total = self.grad[at].astype(F32) + landed[1].astype(F32)
        self.grad[at] = (total + landed[2].astype(F32)).astype(BF)
        self.reduce(j, mid, (large,), self.r_mid[j], ("rm", j), 4)

    def rmm(self, j):
        self.pass_on(SCATTER[j][1], self.r_mid[j], ("rm", j))

    def rs(self, j):
        self.finish(("rm", j))
        large, mid, small = SCATTER[j]
        chosen = {large: self.place(large), mid: self.place(mid)}
        at = where(j, chosen)
        landed = self.r_mid[j]
        total = self.grad[at].astype(F32) + landed[1].astype(F32)
        self.grad[at] = (total + landed[2].astype(F32)).astype(BF)
        n = self.fresh()
        for by in (1, 3, 2):
            at = where(j, {**chosen, small: self.place(small, by)})
            self.copy(self.grad.at[at], self.r_small.at[j, by - 1], self.peer(small, by), n, 5)
        self.live["rs", j] = (n, self.r_small.at[j])

    def rz(self, j):
        self.finish(("rs", j))
        total = self.grad[where(j, {a: self.place(a) for a in AXES})].astype(F32)
        for s in range(3):
            total += self.r_small[j, s].astype(F32)
        self.summed[:, 128 * j : 128 * (j + 1)] = total

    def fin(self):
        total = self.summed[...]
        squares = jnp.sum(total * total, axis=(0, 1), keepdims=True)
        self.norm_src[0] = jnp.broadcast_to(squares, (8, 128))
        self.norm_last = self.fresh()
        to = [self.partner()]
        to += [self.peer("y", by) for by in (1, 2, 3)] + [self.across(by) for by in (1, 2, 3)]
        for slot, device in enumerate(to):
            self.copy(self.norm_src.at[0], self.norm_in.at[slot], device, self.norm_last)
        piece = self.place("y")[0] * 2 + self.place("z")[0]
        for i in range(4):
            self.pieces[i] = self.summed[OWN * i : OWN * (i + 1), :]
            self.exchange(
                self.pieces.at[i], self.shard.at[piece], self.fin_recv.at[piece], self.owner_place(i)
            )

    def norm_total(self, k):
        total = self.norm_src[k - 1]
        first, count = (0, 7) if k == 1 else (3 * k + 1, 3)
        self.take(self.norm_in.at[pl.ds(first, count)], self.norm_last)
        for s in range(count):
            total += self.norm_in[first + s]
        return total

    def n(self, k):
        self.norm_src[k] = self.norm_total(k)
        axis = AXES[k]
        self.norm_last = self.fresh()
        for by in (1, 2, 3):
            to = self.norm_in.at[3 * k + 3 + by]
            self.copy(self.norm_src.at[k], to, self.peer(axis, by), self.norm_last, 5 + k)

    def end(self):
        self.norm_src[3] = self.norm_total(3)
        out = pltpu.make_async_copy(self.norm_src.at[3], self.norm, self.load_sem.at[4])
        out.start()
        for q in range(4):
            self.exchanged(self.pieces.at[0], self.shard.at[q], self.fin_recv.at[q])
        out.wait()


def kernel(*refs):
    body = Body(refs)
    body.run()
    assert body.used == RECEIVES and body.singles == SENDS, (body.used, body.singles)


def update(*refs):
    dx, *shard_in, dx_out, new_master, new_one, new_two = refs[:10]
    held, *held_in, put_master, put_one, put_two, into_sem, out_sem, small_in, small_out = refs[10:]
    parts = 8
    rows = [pl.ds(TOK // parts * i, TOK // parts) for i in range(parts)]
    into = [pltpu.make_async_copy(dx.at[rows[i]], held.at[i], into_sem.at[i]) for i in range(parts)]
    out = [pltpu.make_async_copy(held.at[i], dx_out.at[rows[i]], out_sem.at[i]) for i in range(parts)]
    loads = [pltpu.make_async_copy(a, b, small_in.at[i]) for i, (a, b) in enumerate(zip(shard_in, held_in))]
    for c in loads[:2] + into[:4] + loads[2:] + into[4:]:
        c.start()
    shard, norm, master, one, two = held_in
    for c in loads[:2]:
        c.wait()
    for i in range(4):
        into[i].wait()
        out[i].start()
    limit = jnp.sqrt(jnp.float32(DIN * DOUT))
    clip = jnp.minimum(1.0, limit / (jnp.sqrt(norm[0:1, 0:1]) + 1e-06))
    for i in range(4, parts):
        into[i].wait()
        out[i].start()
    for c in loads[2:]:
        c.wait()
    for q in range(4):
        for j in range(CHUNKS):
            cols = slice(512 * j + 128 * q, 512 * j + 128 * (q + 1))
            clipped = shard[q, :, 128 * j : 128 * (j + 1)] * clip
            weight = master[:, cols]
            first = 0.9 * one[:, cols] + 0.1 * clipped
            second = 0.999 * two[:, cols] + 0.001 * clipped * clipped
            first_hat = first / (1.0 - 0.9**STEP)
            second_hat = second / (1.0 - 0.999**STEP)
            put_one[:, cols] = first
            put_two[:, cols] = second
            put_master[:, cols] = weight - 0.01 * (
                first_hat / (jnp.sqrt(second_hat) + 1e-08) + 0.1 * weight
            )
    for i, (a, b) in enumerate(((put_one, new_one), (put_two, new_two), (put_master, new_master))):
        c = pltpu.make_async_copy(a, b, small_out.at[i])
        c.start()
        out.append(c)
    for c in out:
        c.wait()


def on_device(attn_out, out_grad, master, moment_one, moment_two):
    anywhere = pl.BlockSpec(memory_space=pl.ANY)
    vmem = pl.BlockSpec(memory_space=pltpu.VMEM)
    dx, shard, norm = pl.pallas_call(
        kernel,
        out_shape=(
            jax.ShapeDtypeStruct((TOK, DIN), BF),
            jax.ShapeDtypeStruct((4, OWN, WIDE), F32),
            jax.ShapeDtypeStruct((8, 128), F32),
        ),
        in_specs=[anywhere] * 3,
        out_specs=(anywhere,) * 3,
        scratch_shapes=[
            pltpu.VMEM((2, TOK, HALF), BF),
            pltpu.VMEM((2, HALF, TOK), BF),
            pltpu.VMEM((2 * TOK, DOUT), BF),
            pltpu.VMEM((CHUNKS, HALF, 512), F32),
            pltpu.VMEM((CHUNKS, 2, 2, 4, 2, 2, ROWS, 128), BF),
            pltpu.VMEM((CHUNKS, 2, 2, 4, 2, 2, ROWS, 128), BF),
            pltpu.VMEM((CHUNKS, 3, ROWS, 128), BF),
            pltpu.VMEM((2 * TOK, HALF), F32),
            pltpu.VMEM((OWN, DOUT), F32),
            pltpu.VMEM((4, OWN, WIDE), BF),
            pltpu.VMEM((4, OWN, WIDE), BF),
            pltpu.VMEM((ROWS, WIDE), F32),
            pltpu.VMEM((ROWS, WIDE), F32),
            pltpu.VMEM((4, OWN, WIDE), F32),
            pltpu.VMEM((4, 8, 128), F32),
            pltpu.VMEM((13, 8, 128), F32),
            pltpu.SemaphoreType.DMA((8,)),
            pltpu.SemaphoreType.DMA((8,)),
            pltpu.SemaphoreType.DMA((SENDS,)),
            pltpu.SemaphoreType.DMA((RECEIVES,)),
            pltpu.SemaphoreType.DMA((4,)),
            pltpu.SemaphoreType.DMA((4,)),
            *(pltpu.VMEM(landing_shape(axes[:1]), BF) for axes in SCATTER),
            *(pltpu.VMEM(landing_shape(axes[:2]), BF) for axes in SCATTER),
        ],
        compiler_params=pltpu.CompilerParams(
            collective_id=0, has_side_effects=True, vmem_limit_bytes=66_000_000
        ),
        cost_estimate=pl.CostEstimate(
            flops=4 * TOK * DIN * DOUT, bytes_accessed=40_000_000, transcendentals=0
        ),
        name="step",
    )(attn_out, out_grad, master)
    part = jax.ShapeDtypeStruct((OWN, DOUT), F32)
    row = pltpu.VMEM((OWN, DOUT), F32)
    return pl.pallas_call(
        update,
        out_shape=(jax.ShapeDtypeStruct((TOK, DIN), BF), part, part, part),
        in_specs=[anywhere] * 6,
        out_specs=(anywhere,) * 4,
        scratch_shapes=[
            pltpu.VMEM((8, TOK // 8, DIN), BF),
            pltpu.VMEM((4, OWN, WIDE), F32),
            pltpu.VMEM((8, 128), F32),
            *(row,) * 6,
            pltpu.SemaphoreType.DMA((8,)),
            pltpu.SemaphoreType.DMA((8,)),
            pltpu.SemaphoreType.DMA((5,)),
            pltpu.SemaphoreType.DMA((3,)),
        ],
        name="update",
    )(dx, shard, norm, master, moment_one, moment_two)


def solution(mesh):
    split = P(("seq", "batch"), None)
    return jax.shard_map(
        on_device, mesh=mesh, in_specs=(split,) * 5, out_specs=(split,) * 4, check_vma=False
    )
```

```python
import jax
import jax.numpy as jnp
from jax import lax
from jax.experimental import pallas as pl
from jax.experimental.pallas import tpu as pltpu
from jax.sharding import PartitionSpec as P

DIN = 2560
DOUT = 2560
STEP = 10
TOK = 512
HALF = DIN // 2
ROWS = 80
CHUNKS = 5
OWN = 20
WIDE = 640
BF = jnp.bfloat16
F32 = jnp.float32
MESH = pl.DeviceIdType.MESH
RECEIVES = 83
SENDS = 25
AXES = ("y", "x", "z")
SPLITS = ("x", "z", "y")

GATHER = (("x", "y", "z"), ("y", "z", "x"), ("z", "y", "x"), ("x", "z", "y"), ("y", "z", "x"))
SCATTER = (("z", "y", "x"), ("x", "y", "z"), ("y", "z", "x"), ("z", "y", "x"), ("x", "z", "y"))

ORDER = (
    ("p1", 2), ("p1", 1), ("p1", 4), ("p1", 0), ("tr2",), ("rh", 0), ("pre",), ("ags", 3), ("ags", 1),
    ("rh", 2), ("ags", 2), ("rh", 1), ("p1", 3), ("rhm", 0), ("agm", 2), ("rhm", 1), ("rhm", 2), ("agm", 1),
    ("ags", 0), ("agm", 3), ("rm", 0), ("ags", 4), ("agmf", 1), ("rh", 3), ("rh", 4), ("agmf", 2), ("rmm", 0),
    ("rm", 1), ("agm", 0), ("agmf", 3), ("agh", 1), ("rhm", 3), ("rhm", 4), ("rm", 2), ("rmm", 1), ("rs", 0),
    ("agh", 3), ("rm", 4), ("agm", 4), ("agmf", 0), ("rm", 3), ("rmm", 2), ("aghf", 1), ("rmm", 4), ("aghf", 3),
    ("agmf", 4), ("rs", 1), ("agh", 2), ("rmm", 3), ("rs", 4), ("agh", 4), ("rs", 2), ("rs", 3), ("rz", 0),
    ("rz", 1), ("agh", 0), ("dx", 1), ("aghf", 2), ("rz", 2), ("rz", 3), ("rz", 4), ("fin",), ("aghf", 4),
    ("aghf", 0), ("dx", 3), ("n", 1), ("dx", 2), ("dx", 4), ("n", 2), ("dx", 0), ("end",),
)


def where(chunk, chosen):
    every = pl.ds(0, 2)
    y_col, y_row = chosen.get("y", (every, every))
    z_col, z_row = chosen.get("z", (every, every))
    return (chunk, y_col, z_col, chosen.get("x", pl.ds(0, 4)), z_row, y_row)


DIMS = (("y", 0, 2), ("z", 0, 2), ("x", 0, 4), ("z", 1, 2), ("y", 1, 2))


def landing_shape(gone):
    return (3, *(size for axis, _, size in DIMS if axis not in gone), ROWS, 128)


def halves(axis):
    if axis == "x":
        return pl.ds(0, 2), pl.ds(2, 2)
    return (pl.ds(0, 2), pl.ds(0, 1)), (pl.ds(0, 2), pl.ds(1, 1))


class Body:
    def __init__(self, refs):
        (
            self.attn, self.og, self.master,
            self.dx, self.shard, self.norm,
            self.attn_v, self.attn_t, self.og_v, self.acc, self.grad, self.full, self.r_small, self.dx_acc,
            self.mst, self.give_w, self.stage, self.block, self.summed, self.pieces,
            self.norm_src, self.norm_in,
            self.load_sem, self.send, self.single, self.recv, self.pre_recv, self.fin_recv,
            *landings,
        ) = refs
        self.r_large, self.r_mid = landings[:CHUNKS], landings[CHUNKS:]
        self.used = 0
        self.singles = 0
        self.sent = []
        self.late = []
        self.live = {}
        seq = lax.axis_index("seq")
        batch = lax.axis_index("batch")
        self.zh = seq // 4
        self.core = batch % 2
        self.zl = batch // 8
        self.at = {"x": seq % 4, "y": (batch // 2) % 4, "z": self.zh * 2 + self.zl}

    def device(self, x, y, z, core):
        return ((z // 2) * 4 + x, ((z % 2) * 4 + y) * 2 + core)

    def shifted(self, axis, by):
        return (self.at[axis] + by) % 4

    def peer(self, axis, by):
        place = dict(self.at)
        place[axis] = self.shifted(axis, by)
        return self.device(place["x"], place["y"], place["z"], self.core)

    def across(self, by):
        return self.device(self.at["x"], self.shifted("y", by), self.at["z"], 1 - self.core)

    def partner(self):
        return self.device(self.at["x"], self.at["y"], self.at["z"], 1 - self.core)

    def place(self, axis, by=0):
        at = self.shifted(axis, by)
        if axis == "x":
            return at
        if axis == "y":
            return (at % 2, at // 2)
        turned = (at + 2 * self.core) % 4
        col = turned // 2
        return (col, turned + col * (3 - 2 * turned))

    def fresh(self):
        self.used += 1
        return self.used - 1

    def own_send(self):
        self.singles += 1
        return self.single.at[self.singles - 1]

    def copy(self, src, dst, device, recv=None, group=None):
        n = self.fresh() if recv is None else recv
        c = pltpu.make_async_remote_copy(
            src_ref=src, dst_ref=dst,
            send_sem=self.own_send() if group is None else self.send.at[group],
            recv_sem=self.recv.at[n], device_id=device, device_id_type=MESH,
        )
        c.start()
        if group is None:
            self.sent.append(c)
        return c

    def take(self, like, n):
        self.exchanged(like, like, self.recv.at[n])

    def drain(self):
        for group in range(8):
            blocks = self.full.at[:, :, :, pl.ds(0, 3)]
            if group % 3 == 1:
                blocks = self.full.at[:, pl.ds(0, 1), pl.ds(0, 1), pl.ds(0, 3)]
            if group % 3 == 2:
                one = pl.ds(0, 1)
                blocks = self.full.at[:, one, one, pl.ds(0, 3), one, one]
            if group > 5:
                blocks = self.norm_in.at[pl.ds(1, 3)]
            pltpu.make_async_remote_copy(
                src_ref=blocks, dst_ref=blocks, send_sem=self.send.at[group], recv_sem=self.recv.at[0],
                device_id=self.partner(), device_id_type=MESH,
            ).wait_send()

    def worker_place(self, q):
        z_col = q % 2
        turned = self.zl if z_col == 0 else 3 - self.zl
        return 2 * (self.at["y"] // 2) + q // 2, (turned + 2 * self.zh) % 4, self.zh

    def owner_place(self, i):
        z_row = self.place("z")[1]
        return 2 * (self.at["y"] // 2) + i // 2, 2 * self.core + z_row, i % 2

    def exchange(self, src, dst, recv, place):
        y, z, core = place
        away = pltpu.make_async_remote_copy(
            src_ref=src, dst_ref=dst, send_sem=self.own_send(), recv_sem=recv,
            device_id=self.device(self.at["x"], y, z, core), device_id_type=MESH,
        )
        here = pltpu.make_async_copy(src, dst, recv)
        mine = (y == self.at["y"]) & (z == self.at["z"]) & (core == self.core)
        pl.when(mine)(here.start)
        pl.when(jnp.logical_not(mine))(away.start)
        self.late.append((jnp.logical_not(mine), away))

    def exchanged(self, like, dst, recv):
        pltpu.make_async_remote_copy(
            src_ref=like, dst_ref=dst, send_sem=self.single.at[0], recv_sem=recv,
            device_id=self.partner(), device_id_type=MESH,
        ).wait_recv()

    def run(self):
        half = pl.multiple_of(self.core * HALF, 128)
        other = pl.multiple_of((1 - self.core) * HALF, 128)
        loads = [
            pltpu.make_async_copy(self.master, self.mst, self.load_sem.at[0]),
            pltpu.make_async_copy(self.attn.at[:, pl.ds(half, HALF)], self.attn_v.at[0], self.load_sem.at[1]),
            pltpu.make_async_copy(self.og, self.og_v.at[pl.ds(0, TOK)], self.load_sem.at[2]),
        ]
        barrier = pltpu.get_barrier_semaphore()
        greeted = [self.partner()] + [self.across(by) for by in (1, 2, 3)]
        for axis in AXES:
            greeted += [self.peer(axis, by) for by in (1, 2, 3)]
        for q in range(4):
            for place in (self.worker_place(q), self.owner_place(q)):
                greeted.append(self.device(self.at["x"], *place))
        for device in reversed(greeted):
            pl.semaphore_signal(barrier, inc=1, device_id=device, device_id_type=MESH)
        for load in loads:
            load.start()
        loads[0].wait()
        for q in range(4):
            self.give_w[q] = jnp.concatenate(
                [self.mst[:, 512 * j + 128 * q : 512 * j + 128 * (q + 1)] for j in range(CHUNKS)], axis=1
            ).astype(BF)
        loads[1].wait()
        self.transpose(0)
        pl.semaphore_wait(barrier, len(greeted))

        part = HALF // 2
        self.swap_attn = [
            self.copy(
                self.attn.at[:, pl.ds(pl.multiple_of(other + part * i, 128), part)],
                self.attn_v.at[1, :, pl.ds(part * i, part)],
                self.partner(),
            )
            for i in range(2)
        ]
        slot = (self.at["y"] % 2) * 2 + self.core
        for q in range(4):
            self.exchange(
                self.give_w.at[q], self.stage.at[slot], self.pre_recv.at[slot], self.worker_place(q)
            )
        self.swap_og = [
            self.copy(
                self.og.at[:, pl.ds(512 * j, 512)], self.og_v.at[pl.ds(TOK, TOK), pl.ds(512 * j, 512)],
                self.partner(),
            )
            for j in range(CHUNKS)
        ]
        loads[2].wait()

        sums = [step for step in ORDER if step[0] == "dx"]
        for step in ORDER:
            name = step[0]
            if step == sums[0]:
                name = "dx_first"
            elif step == sums[-1]:
                name = "dx_last"
            elif step in sums:
                name = "dx_more"
            getattr(self, name)(*step[1:])

        self.drain()
        for c in self.sent:
            c.wait_send()
        for go, c in self.late:
            pl.when(go)(c.wait_send)

    def transpose(self, which, first=0, last=10):
        def body(i, carry):
            lanes = pl.ds(pl.multiple_of(i * 128, 128), 128)
            self.attn_t[which, lanes, :] = self.attn_v[which, :, lanes].T
            return carry

        lax.fori_loop(first, last, body, 0)

    def tr2(self):
        for i in range(2):
            self.swap_attn[i].wait_recv()
            self.transpose(1, 5 * i, 5 * i + 5)

    def p1(self, j):
        self.acc[j] = jnp.dot(
            self.attn_t[0], self.og_v[pl.ds(0, TOK), pl.ds(512 * j, 512)], preferred_element_type=F32
        )

    def pre(self):
        for s in range(4):
            self.exchanged(self.give_w.at[0], self.stage.at[s], self.pre_recv.at[s])
            self.block[OWN * s : OWN * (s + 1), :] = self.stage[s].astype(F32)
        here = {axis: self.place(axis) for axis in AXES}
        for j in range(CHUNKS):
            self.full[where(j, here)] = self.block[:, 128 * j : 128 * (j + 1)].astype(BF)

    def ags(self, j):
        axis = GATHER[j][2]
        here = self.full.at[where(j, {a: self.place(a) for a in AXES})]
        n = self.fresh()
        for by in (1, 3, 2):
            self.copy(here, here, self.peer(axis, by), n, 2)
        self.live["ags", j] = (n, self.r_small.at[j])

    def ring(self, j, axis, fixed, key, group, both):
        chosen = {a: self.place(a) for a in fixed}
        split = next(a for a in SPLITS if a != axis and a not in chosen)
        first, second = halves(split)

        def part(by, rows):
            return self.full.at[where(j, {**chosen, axis: self.place(axis, by), split: rows})]

        ahead, behind = self.peer(axis, 1), self.peer(axis, 3)
        n = self.fresh()
        top_ahead = self.copy(part(0, first), part(0, first), ahead, None, group)
        low_behind = self.copy(part(0, second), part(0, second), behind, None, group)
        self.copy(part(0, second), part(0, second), ahead, n, group)
        self.copy(part(0, first), part(0, first), behind, n, group)
        self.live[key] = (top_ahead, low_behind, part, first, second, n, group, both)

    def forward(self, axis, key):
        top_ahead, low_behind, part, first, second, n, group, both = self.live[key]
        top_ahead.wait_recv()
        self.copy(part(3, first), part(3, first), self.peer(axis, 1), n, group)
        low_behind.wait_recv()
        self.copy(part(1, second), part(1, second), self.peer(axis, 3), n, group)
        self.live[key] = (n, both)

    def finish(self, key):
        n, like = self.live[key]
        self.take(like, n)

    def agm(self, j):
        self.finish(("ags", j))
        self.ring(j, GATHER[j][1], (GATHER[j][0],), ("agm", j), 1, self.r_mid[j].at[pl.ds(0, 2)])

    def agmf(self, j):
        self.forward(GATHER[j][1], ("agm", j))

    def agh(self, j):
        self.finish(("agm", j))
        self.ring(j, GATHER[j][0], (), ("agh", j), 0, self.r_large[j].at[pl.ds(0, 2)])

    def aghf(self, j):
        self.forward(GATHER[j][0], ("agh", j))

    def dx_dot(self, j, rows, first=0, last=HALF):
        left = self.og_v[rows, pl.ds(512 * j, 512)]
        right = jnp.concatenate(
            [self.full[j, q // 2, q % 2].reshape(HALF, 128)[first:last] for q in range(4)], axis=1
        )
        return lax.dot_general(left, right, (((1,), (1,)), ((), ())), preferred_element_type=F32)

    def dx_first(self, j):
        self.finish(("agh", j))
        self.dx_acc[...] = self.dx_dot(j, pl.ds(0, 2 * TOK))

    def dx_more(self, j):
        self.finish(("agh", j))
        self.dx_acc[...] += self.dx_dot(j, pl.ds(0, 2 * TOK))

    def dx_last(self, j):
        self.finish(("agh", j))
        start = self.core * HALF
        gives, keeps = [], []
        for which, rows in ((1, pl.ds(TOK, TOK)), (0, pl.ds(0, TOK))):
            for i, (first, last) in enumerate(((0, 512), (512, 1024), (1024, HALF))):
                cols = pl.ds(first, last - first)
                done = self.dx_acc[rows, cols] + self.dx_dot(j, rows, first, last)
                self.attn_v[which, :, cols] = done.astype(BF)
                src = self.attn_v.at[which, :, cols]
                to = self.dx.at[:, pl.ds(pl.multiple_of(start + first, 128), last - first)]
                if which:
                    gives.append(self.copy(src, to, self.partner()))
                else:
                    keep = pltpu.make_async_copy(src, to, self.load_sem.at[5 + i])
                    keep.start()
                    keeps.append(keep)
        for c in gives:
            c.wait_recv()
        for c in keeps:
            c.wait()

    def rh(self, j):
        self.swap_og[j].wait_recv()
        v = self.acc[j] + jnp.dot(
            self.attn_t[1], self.og_v[pl.ds(TOK, TOK), pl.ds(512 * j, 512)], preferred_element_type=F32
        )
        v = v.astype(BF)
        for q in range(4):
            self.grad[j, q // 2, q % 2] = v[:, 128 * q : 128 * (q + 1)].reshape(4, 2, 2, ROWS, 128)
        self.reduce(j, SCATTER[j][0], (), self.r_large[j], ("rh", j), 3)

    def reduce(self, j, axis, fixed, landing, key, group):
        chosen = {a: self.place(a) for a in fixed}
        split = next(a for a in SPLITS if a != axis and a not in chosen)
        first, second = halves(split)
        ahead, behind = self.peer(axis, 1), self.peer(axis, 3)

        def part(by, rows):
            return where(j, {**chosen, axis: self.place(axis, by), split: rows})

        def land(slot, rows):
            index = [slot]
            for a, k, size in DIMS:
                if a == split:
                    index.append(rows if a == "x" else rows[k])
                elif a != axis and a not in chosen:
                    index.append(pl.ds(0, size))
            return tuple(index)

        n = self.fresh()

        def send(by, rows, slot, device, recv):
            return self.copy(
                self.grad.at[part(by, rows)], landing.at[land(slot, rows)], device, recv, group
            )

        far_ahead = send(2, first, 0, ahead, None)
        far_behind = send(2, second, 0, behind, None)
        send(1, second, 1, ahead, n)
        send(3, first, 2, behind, n)
        self.live[key] = (far_ahead, far_behind, part, land, first, second, n, send)

    def pass_on(self, axis, landing, key):
        far_ahead, far_behind, part, land, first, second, n, send = self.live[key]
        far_ahead.wait_recv()
        at = part(1, first)
        self.grad[at] = (self.grad[at].astype(F32) + landing[land(0, first)].astype(F32)).astype(BF)
        send(1, first, 1, self.peer(axis, 1), n)
        far_behind.wait_recv()
        at = part(3, second)
        self.grad[at] = (self.grad[at].astype(F32) + landing[land(0, second)].astype(F32)).astype(BF)
        send(3, second, 2, self.peer(axis, 3), n)
        self.live[key] = (n, landing.at[pl.ds(0, 2)])

    def rhm(self, j):
        self.pass_on(SCATTER[j][0], self.r_large[j], ("rh", j))

    def rm(self, j):
        self.finish(("rh", j))
        large, mid, small = SCATTER[j]
        at = where(j, {large: self.place(large)})
        landed = self.r_large[j]
        total = self.grad[at].astype(F32) + landed[1].astype(F32)
        self.grad[at] = (total + landed[2].astype(F32)).astype(BF)
        self.reduce(j, mid, (large,), self.r_mid[j], ("rm", j), 4)

    def rmm(self, j):
        self.pass_on(SCATTER[j][1], self.r_mid[j], ("rm", j))

    def rs(self, j):
        self.finish(("rm", j))
        large, mid, small = SCATTER[j]
        chosen = {large: self.place(large), mid: self.place(mid)}
        at = where(j, chosen)
        landed = self.r_mid[j]
        total = self.grad[at].astype(F32) + landed[1].astype(F32)
        self.grad[at] = (total + landed[2].astype(F32)).astype(BF)
        n = self.fresh()
        for by in (1, 3, 2):
            at = where(j, {**chosen, small: self.place(small, by)})
            self.copy(self.grad.at[at], self.r_small.at[j, by - 1], self.peer(small, by), n, 5)
        self.live["rs", j] = (n, self.r_small.at[j])

    def rz(self, j):
        self.finish(("rs", j))
        total = self.grad[where(j, {a: self.place(a) for a in AXES})].astype(F32)
        for s in range(3):
            total += self.r_small[j, s].astype(F32)
        self.summed[:, 128 * j : 128 * (j + 1)] = total

    def fin(self):
        total = self.summed[...]
        squares = jnp.sum(total * total, axis=(0, 1), keepdims=True)
        self.norm_src[0] = jnp.broadcast_to(squares, (8, 128))
        self.norm_last = self.fresh()
        to = [self.partner()]
        to += [self.peer("y", by) for by in (1, 2, 3)] + [self.across(by) for by in (1, 2, 3)]
        for slot, device in enumerate(to):
            self.copy(self.norm_src.at[0], self.norm_in.at[slot], device, self.norm_last)
        piece = self.place("y")[0] * 2 + self.place("z")[0]
        for i in range(4):
            self.pieces[i] = self.summed[OWN * i : OWN * (i + 1), :]
            self.exchange(
                self.pieces.at[i], self.shard.at[piece], self.fin_recv.at[piece], self.owner_place(i)
            )

    def norm_total(self, k):
        total = self.norm_src[k - 1]
        first, count = (0, 7) if k == 1 else (3 * k + 1, 3)
        self.take(self.norm_in.at[pl.ds(first, count)], self.norm_last)
        for s in range(count):
            total += self.norm_in[first + s]
        return total

    def n(self, k):
        self.norm_src[k] = self.norm_total(k)
        axis = AXES[k]
        self.norm_last = self.fresh()
        for by in (1, 2, 3):
            to = self.norm_in.at[3 * k + 3 + by]
            self.copy(self.norm_src.at[k], to, self.peer(axis, by), self.norm_last, 5 + k)

    def end(self):
        self.norm_src[3] = self.norm_total(3)
        out = pltpu.make_async_copy(self.norm_src.at[3], self.norm, self.load_sem.at[4])
        out.start()
        for q in range(4):
            self.exchanged(self.pieces.at[0], self.shard.at[q], self.fin_recv.at[q])
        out.wait()


def kernel(*refs):
    body = Body(refs)
    body.run()
    assert body.used == RECEIVES and body.singles == SENDS, (body.used, body.singles)


def update(*refs):
    dx, *shard_in, dx_out, new_master, new_one, new_two = refs[:10]
    held, *held_in, put_master, put_one, put_two, into_sem, out_sem, small_in, small_out = refs[10:]
    parts = 8
    rows = [pl.ds(TOK // parts * i, TOK // parts) for i in range(parts)]
    into = [pltpu.make_async_copy(dx.at[rows[i]], held.at[i], into_sem.at[i]) for i in range(parts)]
    out = [pltpu.make_async_copy(held.at[i], dx_out.at[rows[i]], out_sem.at[i]) for i in range(parts)]
    loads = [pltpu.make_async_copy(a, b, small_in.at[i]) for i, (a, b) in enumerate(zip(shard_in, held_in))]
    for c in loads[:2] + into[:4] + loads[2:] + into[4:]:
        c.start()
    shard, norm, master, one, two = held_in
    for c in loads[:2]:
        c.wait()
    for i in range(4):
        into[i].wait()
        out[i].start()
    limit = jnp.sqrt(jnp.float32(DIN * DOUT))
    clip = jnp.minimum(1.0, limit / (jnp.sqrt(norm[0:1, 0:1]) + 1e-06))
    for i in range(4, parts):
        into[i].wait()
        out[i].start()
    for c in loads[2:]:
        c.wait()
    for q in range(4):
        for j in range(CHUNKS):
            cols = slice(512 * j + 128 * q, 512 * j + 128 * (q + 1))
            clipped = shard[q, :, 128 * j : 128 * (j + 1)] * clip
            weight = master[:, cols]
            first = 0.9 * one[:, cols] + 0.1 * clipped
            second = 0.999 * two[:, cols] + 0.001 * clipped * clipped
            first_hat = first / (1.0 - 0.9**STEP)
            second_hat = second / (1.0 - 0.999**STEP)
            put_one[:, cols] = first
            put_two[:, cols] = second
            put_master[:, cols] = weight - 0.01 * (
                first_hat / (jnp.sqrt(second_hat) + 1e-08) + 0.1 * weight
            )
    for i, (a, b) in enumerate(((put_one, new_one), (put_two, new_two), (put_master, new_master))):
        c = pltpu.make_async_copy(a, b, small_out.at[i])
        c.start()
        out.append(c)
    for c in out:
        c.wait()


def on_device(attn_out, out_grad, master, moment_one, moment_two):
    anywhere = pl.BlockSpec(memory_space=pl.ANY)
    vmem = pl.BlockSpec(memory_space=pltpu.VMEM)
    dx, shard, norm = pl.pallas_call(
        kernel,
        out_shape=(
            jax.ShapeDtypeStruct((TOK, DIN), BF),
            jax.ShapeDtypeStruct((4, OWN, WIDE), F32),
            jax.ShapeDtypeStruct((8, 128), F32),
        ),
        in_specs=[anywhere] * 3,
        out_specs=(anywhere,) * 3,
        scratch_shapes=[
            pltpu.VMEM((2, TOK, HALF), BF),
            pltpu.VMEM((2, HALF, TOK), BF),
            pltpu.VMEM((2 * TOK, DOUT), BF),
            pltpu.VMEM((CHUNKS, HALF, 512), F32),
            pltpu.VMEM((CHUNKS, 2, 2, 4, 2, 2, ROWS, 128), BF),
            pltpu.VMEM((CHUNKS, 2, 2, 4, 2, 2, ROWS, 128), BF),
            pltpu.VMEM((CHUNKS, 3, ROWS, 128), BF),
            pltpu.VMEM((2 * TOK, HALF), F32),
            pltpu.VMEM((OWN, DOUT), F32),
            pltpu.VMEM((4, OWN, WIDE), BF),
            pltpu.VMEM((4, OWN, WIDE), BF),
            pltpu.VMEM((ROWS, WIDE), F32),
            pltpu.VMEM((ROWS, WIDE), F32),
            pltpu.VMEM((4, OWN, WIDE), F32),
            pltpu.VMEM((4, 8, 128), F32),
            pltpu.VMEM((13, 8, 128), F32),
            pltpu.SemaphoreType.DMA((8,)),
            pltpu.SemaphoreType.DMA((8,)),
            pltpu.SemaphoreType.DMA((SENDS,)),
            pltpu.SemaphoreType.DMA((RECEIVES,)),
            pltpu.SemaphoreType.DMA((4,)),
            pltpu.SemaphoreType.DMA((4,)),
            *(pltpu.VMEM(landing_shape(axes[:1]), BF) for axes in SCATTER),
            *(pltpu.VMEM(landing_shape(axes[:2]), BF) for axes in SCATTER),
        ],
        compiler_params=pltpu.CompilerParams(
            collective_id=0, has_side_effects=True, vmem_limit_bytes=66_000_000
        ),
        cost_estimate=pl.CostEstimate(
            flops=4 * TOK * DIN * DOUT, bytes_accessed=40_000_000, transcendentals=0
        ),
        name="step",
    )(attn_out, out_grad, master)
    part = jax.ShapeDtypeStruct((OWN, DOUT), F32)
    row = pltpu.VMEM((OWN, DOUT), F32)
    return pl.pallas_call(
        update,
        out_shape=(jax.ShapeDtypeStruct((TOK, DIN), BF), part, part, part),
        in_specs=[anywhere] * 6,
        out_specs=(anywhere,) * 4,
        scratch_shapes=[
            pltpu.VMEM((8, TOK // 8, DIN), BF),
            pltpu.VMEM((4, OWN, WIDE), F32),
            pltpu.VMEM((8, 128), F32),
            *(row,) * 6,
            pltpu.SemaphoreType.DMA((8,)),
            pltpu.SemaphoreType.DMA((8,)),
            pltpu.SemaphoreType.DMA((5,)),
            pltpu.SemaphoreType.DMA((3,)),
        ],
        name="update",
    )(dx, shard, norm, master, moment_one, moment_two)


def solution(mesh):
    split = P(("seq", "batch"), None)
    return jax.shard_map(
        on_device, mesh=mesh, in_specs=(split,) * 5, out_specs=(split,) * 4, check_vma=False
    )
```
